32 devices in a mesh: job: 4 (over y, x), zero: 2 (over core), cols: 4 (over z).
Axes of the slice: x: 2, y: 2, z: 4, core: 2. Of those that a mesh axis runs over, the one named last changes fastest.
Arguments:
- weight_gate: bfloat16 [8192, 8192], P(('job', 'zero'), 'cols'), parts along dimension 0, may hold values from -0.1875 to 0.1875
- low_gate: bfloat16 [8192, 32], P(('job', 'zero')), parts along dimension 0, may hold values from -0.125 to 0.125
- high_gate: bfloat16 [128, 8192], P('job', 'cols'), parts along dimension 0, may hold values from -1 to 1
- weight_up: bfloat16 [8192, 8192], P(('job', 'zero'), 'cols'), parts along dimension 0, may hold values from -0.1875 to 0.1875
- low_up: bfloat16 [8192, 32], P(('job', 'zero')), parts along dimension 0, may hold values from -0.125 to 0.125
- high_up: bfloat16 [128, 8192], P('job', 'cols'), parts along dimension 0, may hold values from -1 to 1
- norm_train: float32 [8192], P(('job', 'zero', 'cols')), parts along dimension 0, may hold values from 0.25 to 1.75
- norm_step: float32 [8192], P(('job', 'zero', 'cols')), parts along dimension 0, may hold values from -0.3 to 0.3
Outputs:
- serving_gate: bfloat16 [8192, 8192], P('job', 'cols'), parts along dimension 0
- serving_up: bfloat16 [8192, 8192], P('job', 'cols'), parts along dimension 0
- column_gate: float32 [32768], P(('job', 'cols')), parts along dimension 0
- column_up: float32 [32768], P(('job', 'cols')), parts along dimension 0
- serve_norm: bfloat16 [8192], P('job'), parts along dimension 0
The draws below stay inside these ranges and needn't reach their ends.
There are 4 independent parts, one for each index of `job`. The reference program is written for one: setup_inputs(seed, part) draws one part's arguments, and reference() takes and returns one part's arrays. A program takes and returns all parts, laid end to end along the dimension named above; each array names one. Nothing has to cross between parts.
All inputs are finite; a program needn't handle non-finite values. Where the reference program divides by a largest or mean magnitude, that divisor is 1e-20 or more.
Results may differ from the reference program's by a relative error of at most 0.001.
Values may be sent and summed in bfloat16 or wider, within the bound.
A program may use at most 128 MiB of HBM per device.

```python
import jax
import jax.numpy as jnp

D_MODEL = 2048
D_INNER = 8192
RANK = 32


def raised(array, own_key, source, target, blocks, factor):
    def block_of(position):
        return (jnp.arange(array.shape[position]) // (array.shape[position] // blocks)).reshape((-1,) + (1,) * (array.ndim - 1 - position))

    one_side = jax.random.permutation(own_key, blocks)[block_of(target)]
    second = (block_of(target) + blocks // 2) % blocks
    return jnp.where((block_of(source) == one_side) | (block_of(source) == second), factor * array, array)


def level_of(key, dims, pieces, smallest, largest):
    def one(position, shards_of):
        draws = jax.random.uniform(jax.random.fold_in(jax.random.fold_in(key, 6), position), (shards_of,), jnp.float32, smallest / len(pieces), largest / len(pieces))
        return jnp.repeat(jnp.exp(draws), dims[position] // shards_of).reshape((-1,) + (1,) * (len(dims) - position - 1))

    level = one(*pieces[0])
    for cut in pieces[1:]:
        level = level * one(*cut)
    return level


def normal_values(rng, dims, scale, bound, pieces=(), dtype=jnp.bfloat16):
    entries = scale * jax.random.normal(rng, dims, jnp.float32)
    if pieces:
        entries = entries * level_of(rng, dims, pieces, -0.22, 0.18)
    return jnp.clip(entries, -bound, bound).astype(dtype)


def gaussian_with(own_key, dims, deviation, most, split, heavy, held_as=jnp.bfloat16):
    array = deviation * jax.random.normal(own_key, dims, jnp.float32)
    if split:
        array = array * level_of(own_key, dims, split, -0.22, 0.18)
    return jnp.clip(raised(array, jax.random.fold_in(own_key, 3), *heavy), -most, most).astype(held_as)


def setup_inputs(seed: int = 0, part: int = 0) -> dict:
    keys = jax.random.split(jax.random.key(seed), 9)
    part_keys = jax.random.split(jax.random.fold_in(keys[8], part), 9)
    weight_gate = gaussian_with(part_keys[0], (D_MODEL, D_INNER), D_MODEL ** -0.5, 0.1875, ((0, 2), (1, 4)), (0, 1, 4, 2.0))
    low_gate = normal_values(part_keys[1], (D_MODEL, RANK), D_MODEL ** -0.5, 0.125, ((0, 2),))
    high_gate = normal_values(part_keys[2], (RANK, D_INNER), RANK ** -0.5, 1.0, ((1, 4),))
    weight_up = gaussian_with(part_keys[3], (D_MODEL, D_INNER), D_MODEL ** -0.5, 0.1875, ((0, 2), (1, 4)), (0, 1, 4, 2.0))
    low_up = normal_values(part_keys[4], (D_MODEL, RANK), D_MODEL ** -0.5, 0.125, ((0, 2),))
    high_up = normal_values(part_keys[5], (RANK, D_INNER), RANK ** -0.5, 1.0, ((1, 4),))
    norm_train = jnp.clip(1.0 + 0.15 * jax.random.normal(part_keys[6], (D_MODEL,), jnp.float32), 0.25, 1.75)
    norm_step = jnp.clip(jax.random.uniform(part_keys[7], (D_MODEL,), jnp.float32, -0.3, 0.3) * level_of(part_keys[7], (D_MODEL,), ((0, 8),), -0.4, 0.0), -0.3, 0.3)
    return {"weight_gate": weight_gate, "low_gate": low_gate, "high_gate": high_gate, "weight_up": weight_up, "low_up": low_up, "high_up": high_up, "norm_train": norm_train, "norm_step": norm_step}


mix_rate = 2.0


def reference(weight_gate, low_gate, high_gate, weight_up, low_up, high_up, norm_train, norm_step):
    whole_gate = weight_gate.astype(jnp.float32) + mix_rate * jnp.dot(low_gate, high_gate, preferred_element_type=jnp.float32)
    whole_up = weight_up.astype(jnp.float32) + mix_rate * jnp.dot(low_up, high_up, preferred_element_type=jnp.float32)
    column_gate = jnp.max(jnp.abs(whole_gate), axis=0)
    serving_gate = (whole_gate / column_gate).astype(jnp.bfloat16)
    column_up = jnp.max(jnp.abs(whole_up), axis=0)
    serving_up = (whole_up / column_up).astype(jnp.bfloat16)
    serve_norm = (norm_train + norm_step).astype(jnp.bfloat16)
    return serving_gate, serving_up, column_gate, column_up, serve_norm
```

```python
import functools

import jax
import jax.numpy as jnp
from jax import lax
from jax.experimental import pallas as pl
from jax.experimental.pallas import tpu as pltpu
from jax.sharding import PartitionSpec as P


mix_rate = 2.0
MESH = pl.DeviceIdType.MESH


def first_kernel(zeros, cols, lows, weight_ref, *refs):
    train_ref, step_ref = refs[:2]
    low_refs = refs[2:2 + lows]
    norm_ref = refs[2 + lows]
    got_refs = refs[3 + lows:3 + 2 * lows]
    moved_refs = refs[3 + 2 * lows:2 + 2 * lows + zeros]
    refs = refs[2 + 2 * lows + zeros:]
    landed = refs[:lows]
    mine, slots, norm_send, norm_recv, low_send, low_recv, weight_send, weight_recv = refs[lows:]
    group = zeros * cols
    zero, col = lax.axis_index("zero"), lax.axis_index("cols")
    me = zero * cols + col

    def device(rank):
        return {"zero": rank // cols, "cols": lax.rem(rank, cols)}

    barrier = pltpu.get_barrier_semaphore()
    for s in range(1, group):
        pl.semaphore_signal(barrier, inc=1, device_id=device(lax.rem(me + s, group)), device_id_type=MESH)
    mine[...] = train_ref[...] + step_ref[...]
    pl.semaphore_wait(barrier, group - 1)

    copies = []
    for s in range(1, zeros):
        for k in range(lows):
            copies.append(pltpu.make_async_remote_copy(
                src_ref=low_refs[k], dst_ref=landed[k].at[s - 1],
                send_sem=low_send.at[k, s - 1], recv_sem=low_recv.at[k, s - 1],
                device_id={"zero": lax.rem(zero + s, zeros), "cols": col}, device_id_type=MESH))
            copies[-1].start()
    for s in range(1, zeros):
        copies.append(pltpu.make_async_remote_copy(
            src_ref=weight_ref, dst_ref=moved_refs[s - 1],
            send_sem=weight_send.at[s - 1], recv_sem=weight_recv.at[s - 1],
            device_id={"zero": lax.rem(zero + s, zeros), "cols": col}, device_id_type=MESH))
    for s in range(1, group):
        copy = pltpu.make_async_remote_copy(
            src_ref=mine, dst_ref=slots.at[me],
            send_sem=norm_send.at[s - 1], recv_sem=norm_recv.at[s - 1],
            device_id=device(lax.rem(me + s, group)), device_id_type=MESH)
        copy.start()
        copies.append(copy)
    for copy in copies[lows * (zeros - 1):(1 + lows) * (zeros - 1)]:
        copy.start()
    for k in range(lows):
        got_refs[k][0] = low_refs[k][...].T
    for copy in copies:
        copy.wait()
    for k in range(lows):
        for s in range(1, zeros):
            got_refs[k][s] = landed[k][s - 1].T
    slots[me] = mine[...]
    norm_ref[...] = jnp.concatenate([slots[g] for g in range(group)], axis=0).astype(norm_ref.dtype)


def exchange_first(zeros, cols, weight, train, step, lows):
    group = zeros * cols
    lanes = 128 if train.shape[0] % 128 == 0 else train.shape[0]
    tall = train.shape[0] // lanes
    outs = pl.pallas_call(
        functools.partial(first_kernel, zeros, cols, len(lows)),
        out_shape=[jax.ShapeDtypeStruct((group * tall, lanes), jnp.bfloat16)]
        + [jax.ShapeDtypeStruct((zeros,) + low.shape, low.dtype) for low in lows]
        + [jax.ShapeDtypeStruct(weight.shape, weight.dtype)] * (zeros - 1),
        in_specs=[pl.BlockSpec(memory_space=pl.ANY)] + [pl.BlockSpec(memory_space=pltpu.VMEM)] * (2 + len(lows)),
        out_specs=[pl.BlockSpec(memory_space=pltpu.VMEM)] * (1 + len(lows))
        + [pl.BlockSpec(memory_space=pl.ANY)] * (zeros - 1),
        scratch_shapes=[
            pltpu.VMEM((zeros - 1,) + low.shape[::-1], low.dtype) for low in lows
        ] + [
            pltpu.VMEM((tall, lanes), jnp.float32),
            pltpu.VMEM((group, tall, lanes), jnp.float32),
            pltpu.SemaphoreType.DMA((group - 1,)),
            pltpu.SemaphoreType.DMA((group - 1,)),
            pltpu.SemaphoreType.DMA((len(lows), zeros - 1)),
            pltpu.SemaphoreType.DMA((len(lows), zeros - 1)),
            pltpu.SemaphoreType.DMA((zeros - 1,)),
            pltpu.SemaphoreType.DMA((zeros - 1,)),
        ],
        cost_estimate=pl.CostEstimate(flops=0, bytes_accessed=2 ** 22, transcendentals=0),
        compiler_params=pltpu.CompilerParams(collective_id=0, has_side_effects=True),
    )(weight, train.reshape(tall, lanes), step.reshape(tall, lanes), *[low.T for low in lows])
    return outs[0].reshape(group * tall * lanes), outs[1:1 + len(lows)], outs[1 + len(lows):]


def merge_kernel(zeros, chunk, *refs):
    weight_refs = refs[:zeros]
    low_ref, high_ref, out_ref, column_ref, whole = refs[zeros:]
    zero = lax.axis_index("zero")
    rows, width = weight_refs[0].shape
    high = high_ref[...] * jnp.bfloat16(mix_rate)
    most = jnp.zeros((8, width), jnp.float32)
    for s in range(zeros):
        def step(i, most, s=s):
            at = pl.ds(pl.multiple_of(i * chunk, chunk), chunk)
            low = low_ref[s, at, :]
            value = weight_refs[s][at, :].astype(jnp.float32) + jnp.dot(
                low, high, preferred_element_type=jnp.float32)
            whole[s, at, :] = value
            return jnp.maximum(most, jnp.max(jnp.abs(value).reshape(chunk // 8, 8, width), axis=0))

        most = lax.fori_loop(0, rows // chunk, step, most, unroll=True)
    column = jnp.max(most, axis=0, keepdims=True)
    column_ref[...] = column
    scale = 1.0 / column
    for s in range(zeros):
        base = lax.rem(zero - s + zeros, zeros) * rows

        def put(i, carry, s=s, base=base):
            start = pl.multiple_of(i * chunk, chunk)
            out_ref[pl.ds(pl.multiple_of(base + start, chunk), chunk), :] = (
                whole[s, pl.ds(start, chunk), :] * scale).astype(out_ref.dtype)
            return carry

        lax.fori_loop(0, rows // chunk, put, 0, unroll=True)


def merge(zeros, weights, low, high):
    rows, columns = weights[0].shape
    rank = low.shape[2]
    width = min(512, columns)
    chunk = min(128, rows)
    serving, column = pl.pallas_call(
        functools.partial(merge_kernel, zeros, chunk),
        grid=(columns // width,),
        out_shape=[
            jax.ShapeDtypeStruct((rows * zeros, columns), jnp.bfloat16),
            jax.ShapeDtypeStruct((1, columns), jnp.float32),
        ],
        in_specs=[pl.BlockSpec((rows, width), lambda j: (0, j))] * zeros + [
            pl.BlockSpec((zeros, rows, rank), lambda j: (0, 0, 0)),
            pl.BlockSpec((rank, width), lambda j: (0, j)),
        ],
        out_specs=[
            pl.BlockSpec((rows * zeros, width), lambda j: (0, j)),
            pl.BlockSpec((1, width), lambda j: (0, j)),
        ],
        scratch_shapes=[pltpu.VMEM((zeros, rows, width), jnp.float32)],
        cost_estimate=pl.CostEstimate(
            flops=2 * rows * zeros * columns * rank,
            bytes_accessed=4 * rows * zeros * columns, transcendentals=0),
        compiler_params=pltpu.CompilerParams(dimension_semantics=("arbitrary",), vmem_limit_bytes=60 * 2 ** 20),
    )(*weights, low, high)
    return serving, column.reshape(columns)


def plain(zeros, cols, weight_gate, low_gate, high_gate, weight_up, low_up, high_up, norm_train, norm_step):
    def moved(array):
        return [array] + [
            lax.ppermute(array, "zero", [(i, (i + s) % zeros) for i in range(zeros)])
            for s in range(1, zeros)
        ]

    serve_norm, (all_gate, all_up), gates = exchange_first(
        zeros, cols, weight_gate, norm_train, norm_step, (low_gate, low_up))
    weight_up, all_up = lax.optimization_barrier((weight_up, all_up))
    ups = moved(weight_up)
    serving_gate, column_gate = merge(zeros, [weight_gate, *gates], all_gate, high_gate)
    serving_up, column_up = merge(zeros, ups, all_up, high_up)
    return (serving_gate, serving_up, column_gate, column_up, serve_norm)


def local_kernel(zeros, cols, width, chunk, gate_ref, up_ref, low_gate_ref, low_up_ref, high_gate_ref, high_up_ref,
                 train_ref, step_ref, whole_gate, whole_up, column_gate, column_up, norm_ref,
                 raw, lows, lows_t, highs, own, other, passed, mine, parts, slots,
                 weight_sems, small_sems, norm_sems, norm_send, norm_recv, own_send, passed_recv, pass_send, other_recv,
                 hand_send, hand_recv):
    zero, col = lax.axis_index("zero"), lax.axis_index("cols")
    group = zeros * cols
    me = zero * cols + col
    pair = col + 1 - 2 * lax.rem(col, 2)
    top = zeros - 1
    rows, columns = raw.shape[1:]
    wholes = (whole_gate, whole_up)

    barrier = pltpu.get_barrier_semaphore()
    for s in range(1, cols):
        for z in range(zeros):
            pl.semaphore_signal(barrier, inc=1, device_id={"zero": z, "cols": lax.rem(col + s, cols)}, device_id_type=MESH)

    small = []
    for k, (low, high) in enumerate(((low_gate_ref, high_gate_ref), (low_up_ref, high_up_ref))):
        small.append(pltpu.make_async_copy(low, lows_t.at[k], small_sems.at[k, 0]))
        small.append(pltpu.make_async_copy(high, highs.at[k], small_sems.at[k, 1]))
    pieces = columns // width
    loads = [[], []]
    for k, weight in enumerate((gate_ref, up_ref)):
        small[2 * k].start()
        small[2 * k + 1].start()
        for j in range(pieces):
            at = pl.ds(j * width, width)
            copy = pltpu.make_async_copy(weight.at[:, at], raw.at[k, :, at], weight_sems.at[k, j])
            copy.start()
            loads[k].append(copy)
    norms = [pltpu.make_async_copy(ref, parts.at[i], norm_sems.at[i]) for i, ref in enumerate((train_ref, step_ref))]
    for copy in norms:
        copy.start()

    def column_of(k):
        small[2 * k].wait()
        small[2 * k + 1].wait()
        lows[k] = lows_t[k].T
        for j in range(pieces):
            loads[k][j].wait()
            at = pl.ds(j * width, width)
            high = highs[k, :, at] * jnp.bfloat16(mix_rate)

            def step(i, most):
                here = pl.ds(pl.multiple_of(i * chunk, chunk), chunk)
                value = raw[k, here, at].astype(jnp.float32) + jnp.dot(
                    lows[k, here, :], high, preferred_element_type=jnp.float32)
                wholes[k][here, at] = value
                return jnp.maximum(most, jnp.max(jnp.abs(value).reshape(chunk // 8, 8, width), axis=0))

            most = lax.fori_loop(0, rows // chunk, step, jnp.zeros((8, width), jnp.float32), unroll=True)
            own[k, :, at] = jnp.max(most, axis=0, keepdims=True)

    def send_own(k):
        return pltpu.make_async_remote_copy(
            src_ref=own.at[k], dst_ref=passed.at[k, zero], send_sem=own_send.at[k], recv_sem=passed_recv.at[k, zero],
            device_id={"zero": top, "cols": pair}, device_id_type=MESH)

    def take_own(k, z):
        return pltpu.make_async_remote_copy(
            src_ref=own.at[k], dst_ref=passed.at[k, z], send_sem=own_send.at[k], recv_sem=passed_recv.at[k, z],
            device_id={"zero": top, "cols": pair}, device_id_type=MESH)

    def pass_on(k, z):
        return pltpu.make_async_remote_copy(
            src_ref=passed.at[k, z], dst_ref=other.at[k], send_sem=pass_send.at[k, z], recv_sem=other_recv.at[k],
            device_id={"zero": zeros - 1 - z, "cols": pair}, device_id_type=MESH)

    def send_norm(s, z):
        return pltpu.make_async_remote_copy(
            src_ref=mine, dst_ref=slots.at[me], send_sem=norm_send.at[s - 1, z], recv_sem=norm_recv.at[s - 1, zero],
            device_id={"zero": z, "cols": lax.rem(col + s, cols)}, device_id_type=MESH)

    def take_norm(s, z):
        return pltpu.make_async_remote_copy(
            src_ref=mine, dst_ref=slots.at[z * cols + lax.rem(col - s + cols, cols)],
            send_sem=norm_send.at[s - 1, z], recv_sem=norm_recv.at[s - 1, z],
            device_id={"zero": z, "cols": lax.rem(col + s, cols)}, device_id_type=MESH)

    def hand_on(z):
        slot = slots.at[z * cols + pair]
        return pltpu.make_async_remote_copy(
            src_ref=slot, dst_ref=slot, send_sem=hand_send.at[z], recv_sem=hand_recv,
            device_id={"zero": zeros - 1 - z, "cols": pair}, device_id_type=MESH)

    column_of(0)
    for copy in norms:
        copy.wait()
    mine[...] = parts[0] + parts[1]
    pl.semaphore_wait(barrier, zeros * (cols - 1))
    send_own(0).start()
    for s in range(1, cols):
        for z in range(zeros):
            send_norm(s, z).start()
    column_of(1)
    send_own(1).start()
    for s in range(1, cols):
        for z in range(zeros):
            take_norm(s, z).wait_recv()

    @pl.when(zero == top)
    def _():
        for z in range(zeros):
            take_own(0, z).wait_recv()
            pass_on(0, z).start()
        for z in range(zeros):
            hand_on(z).start()
        for z in range(zeros):
            take_own(1, z).wait_recv()
            pass_on(1, z).start()
        for z in range(zeros):
            pass_on(0, z).wait_send()
            pass_on(1, z).wait_send()
            hand_on(z).wait_send()

    for k in range(2):
        send_own(k).wait_send()
    for s in range(1, cols):
        for z in range(zeros):
            send_norm(s, z).wait_send()
    slots[me] = mine[...]
    pltpu.make_async_remote_copy(
        src_ref=mine, dst_ref=slots.at[(zeros - 1 - zero) * cols + col], send_sem=hand_send.at[0], recv_sem=hand_recv,
        device_id={"zero": zero, "cols": pair}, device_id_type=MESH).wait_recv()
    norm_ref[...] = jnp.concatenate([slots[g] for g in range(group)], axis=0).astype(norm_ref.dtype)
    for k, column in enumerate((column_gate, column_up)):
        pltpu.make_async_remote_copy(
            src_ref=own.at[k], dst_ref=other.at[k], send_sem=own_send.at[k], recv_sem=other_recv.at[k],
            device_id={"zero": zero, "cols": pair}, device_id_type=MESH).wait_recv()
        column[...] = jnp.maximum(own[k], other[k])


def local_part(zeros, cols, gate, up, low_gate, low_up, high_gate, high_up, train, step):
    rows, columns = gate.shape
    rank = low_gate.shape[1]
    group = zeros * cols
    lanes = 128 if train.shape[0] % 128 == 0 else train.shape[0]
    tall = train.shape[0] // lanes
    width = min(512, columns)
    chunk = min(128, rows)
    dma = pltpu.SemaphoreType.DMA
    hbm, vmem = pl.BlockSpec(memory_space=pltpu.HBM), pl.BlockSpec(memory_space=pltpu.VMEM)
    return pl.pallas_call(
        functools.partial(local_kernel, zeros, cols, width, chunk),
        out_shape=[pltpu.VMEM((rows, columns), jnp.float32)] * 2
        + [pltpu.VMEM((1, columns), jnp.float32)] * 2
        + [pltpu.VMEM((group * tall, lanes), jnp.bfloat16)],
        in_specs=[hbm] * 8,
        out_specs=[vmem] * 5,
        scratch_shapes=[
            pltpu.VMEM((2, rows, columns), gate.dtype),
            pltpu.VMEM((2, rows, rank), gate.dtype),
            pltpu.VMEM((2, rank, rows), gate.dtype),
            pltpu.VMEM((2, rank, columns), gate.dtype),
            pltpu.VMEM((2, 1, columns), jnp.float32),
            pltpu.VMEM((2, 1, columns), jnp.float32),
            pltpu.VMEM((2, zeros, 1, columns), jnp.float32),
            pltpu.VMEM((tall, lanes), jnp.float32),
            pltpu.VMEM((2, tall, lanes), jnp.float32),
            pltpu.VMEM((group, tall, lanes), jnp.float32),
            dma((2, columns // width)), dma((2, 2)), dma((2,)),
            dma((cols - 1, zeros)), dma((cols - 1, zeros)),
            dma((2,)), dma((2, zeros)), dma((2, zeros)), dma((2,)),
            dma((zeros,)), dma,
        ],
        cost_estimate=pl.CostEstimate(flops=2 ** 32, bytes_accessed=2 ** 23, transcendentals=0),
        compiler_params=pltpu.CompilerParams(collective_id=0, has_side_effects=True, vmem_limit_bytes=14 * 2 ** 20),
    )(*[pltpu.with_memory_space_constraint(array, pltpu.HBM) for array in (
        gate, up, low_gate.T, low_up.T, high_gate, high_up, train.reshape(tall, lanes), step.reshape(tall, lanes))])


def write_out(value_of, chunks, chunk, stage, sems, out_ref, base, waiting):
    slots = stage.shape[0]
    for i in range(chunks):
        slot = len(waiting) % slots
        if len(waiting) >= slots:
            waiting[-slots].wait()
        stage[slot] = value_of(pl.ds(i * chunk, chunk)).astype(stage.dtype)
        copy = pltpu.make_async_copy(
            stage.at[slot], out_ref.at[pl.ds(pl.multiple_of(base + i * chunk, chunk), chunk), :], sems.at[slot])
        copy.start()
        waiting.append(copy)


def remote_value(raw_ref, low_ref, high, scale):
    def value_of(at):
        return (raw_ref[at, :].astype(jnp.float32) + jnp.dot(
            low_ref[at, :], high, preferred_element_type=jnp.float32)) * scale

    return value_of


def most_kernel(zeros, chunk, whole_gate, whole_up, moved, low_gate_t, low_up_t, high_ref, column_gate, column_up, norm_in,
                gate_out, up_out, column_gate_out, column_up_out, norm_out, low_up, stage, low_gate, sems):
    zero = lax.axis_index("zero")
    rows = moved.shape[0]
    column_gate_out[...] = column_gate[...]
    column_up_out[...] = column_up[...]
    norm_out[...] = norm_in[...]
    high = high_ref[...] * jnp.bfloat16(mix_rate)
    waiting = []
    scale = 1.0 / column_gate[...]
    chunks = rows // chunk
    write_out(lambda at: whole_gate[at, :] * scale, chunks, chunk, stage, sems, gate_out, zero * rows, waiting)
    low_gate[...] = low_gate_t[...].T
    write_out(remote_value(moved, low_gate, high, scale), chunks, chunk, stage, sems, gate_out, (zeros - 1 - zero) * rows, waiting)
    scale = 1.0 / column_up[...]
    write_out(lambda at: whole_up[at, :] * scale, chunks, chunk, stage, sems, up_out, zero * rows, waiting)
    low_up[...] = low_up_t[...].T
    for copy in waiting[-stage.shape[0]:]:
        copy.wait()


def last_kernel(zeros, chunk, moved, low_ref, high_ref, column_ref, up_in, up_out, stage, sems):
    zero = lax.axis_index("zero")
    rows = moved.shape[0]
    waiting = []
    write_out(remote_value(moved, low_ref, high_ref[...] * jnp.bfloat16(mix_rate), 1.0 / column_ref[...]),
              rows // chunk, chunk, stage, sems, up_out, (zeros - 1 - zero) * rows, waiting)
    for copy in waiting[-stage.shape[0]:]:
        copy.wait()


def per_device(zeros, cols, weight_gate, low_gate, high_gate, weight_up, low_up, high_up, norm_train, norm_step):
    if zeros != 2 or cols % 2:
        return plain(zeros, cols, weight_gate, low_gate, high_gate, weight_up, low_up, high_up, norm_train, norm_step)
    rows, columns = weight_gate.shape
    rank = low_gate.shape[1]
    chunk = min(128, rows)

    def moved(array):
        return lax.ppermute(array, "zero", [(i, zeros - 1 - i) for i in range(zeros)])

    far_low_gate, far_low_up = moved(low_gate), moved(low_up)
    far_gate, far_up = moved(weight_gate), moved(weight_up)
    whole_gate, whole_up, column_gate, column_up, norm = local_part(
        zeros, cols, weight_gate, weight_up, low_gate, low_up, high_gate, high_up, norm_train, norm_step)
    hbm, vmem = pl.BlockSpec(memory_space=pltpu.HBM), pl.BlockSpec(memory_space=pltpu.VMEM)
    wide = jax.ShapeDtypeStruct((rows * zeros, columns), jnp.bfloat16)
    line = jax.ShapeDtypeStruct((1, columns), jnp.float32)
    serving_gate, serving_up, column_gate_out, column_up_out, serve_norm, far_low = pl.pallas_call(
        functools.partial(most_kernel, zeros, chunk),
        out_shape=[wide, wide, line, line, jax.ShapeDtypeStruct(norm.shape, norm.dtype),
                   pltpu.VMEM((rows, rank), low_up.dtype)],
        in_specs=[vmem] * 9,
        out_specs=[hbm, hbm] + [vmem] * 4,
        scratch_shapes=[pltpu.VMEM((4, chunk, columns), jnp.bfloat16), pltpu.VMEM((rows, rank), low_gate.dtype),
                        pltpu.SemaphoreType.DMA((4,))],
        cost_estimate=pl.CostEstimate(flops=2 ** 32, bytes_accessed=3 * 2 ** 22, transcendentals=0),
        compiler_params=pltpu.CompilerParams(vmem_limit_bytes=16 * 2 ** 20),
    )(whole_gate, whole_up, far_gate, far_low_gate.T, far_low_up.T, high_gate, column_gate, column_up, norm)
    serving_up = pl.pallas_call(
        functools.partial(last_kernel, zeros, chunk),
        out_shape=wide,
        in_specs=[vmem] * 4 + [hbm],
        out_specs=hbm,
        input_output_aliases={4: 0},
        scratch_shapes=[pltpu.VMEM((4, chunk, columns), jnp.bfloat16), pltpu.SemaphoreType.DMA((4,))],
        cost_estimate=pl.CostEstimate(flops=2 ** 30, bytes_accessed=2 ** 22, transcendentals=0),
        compiler_params=pltpu.CompilerParams(vmem_limit_bytes=16 * 2 ** 20),
    )(far_up, far_low, high_up, column_up, serving_up)
    return (serving_gate, serving_up, column_gate_out.reshape(columns), column_up_out.reshape(columns),
            serve_norm.reshape(zeros * cols * norm_train.shape[0]))


def solution(mesh):
    in_specs = (
        P(("job", "zero"), "cols"),
        P(("job", "zero"), None),
        P("job", "cols"),
        P(("job", "zero"), "cols"),
        P(("job", "zero"), None),
        P("job", "cols"),
        P(("job", "zero", "cols")),
        P(("job", "zero", "cols")),
    )
    out_specs = (
        P("job", "cols"),
        P("job", "cols"),
        P(("job", "cols")),
        P(("job", "cols")),
        P("job"),
    )
    return jax.shard_map(
        functools.partial(per_device, mesh.shape["zero"], mesh.shape["cols"]),
        mesh=mesh, in_specs=in_specs, out_specs=out_specs, check_vma=False
    )
```

```python
import functools

import jax
import jax.numpy as jnp
from jax import lax
from jax.experimental import pallas as pl
from jax.experimental.pallas import tpu as pltpu
from jax.sharding import PartitionSpec as P


mix_rate = 2.0
MESH = pl.DeviceIdType.MESH


def first_kernel(zeros, cols, lows, weight_ref, *refs):
    train_ref, step_ref = refs[:2]
    low_refs = refs[2:2 + lows]
    norm_ref = refs[2 + lows]
    got_refs = refs[3 + lows:3 + 2 * lows]
    moved_refs = refs[3 + 2 * lows:2 + 2 * lows + zeros]
    refs = refs[2 + 2 * lows + zeros:]
    landed = refs[:lows]
    mine, slots, norm_send, norm_recv, low_send, low_recv, weight_send, weight_recv = refs[lows:]
    group = zeros * cols
    zero, col = lax.axis_index("zero"), lax.axis_index("cols")
    me = zero * cols + col

    def device(rank):
        return {"zero": rank // cols, "cols": lax.rem(rank, cols)}

    barrier = pltpu.get_barrier_semaphore()
    for s in range(1, group):
        pl.semaphore_signal(barrier, inc=1, device_id=device(lax.rem(me + s, group)), device_id_type=MESH)
    mine[...] = train_ref[...] + step_ref[...]
    pl.semaphore_wait(barrier, group - 1)

    copies = []
    for s in range(1, zeros):
        for k in range(lows):
            copies.append(pltpu.make_async_remote_copy(
                src_ref=low_refs[k], dst_ref=landed[k].at[s - 1],
                send_sem=low_send.at[k, s - 1], recv_sem=low_recv.at[k, s - 1],
                device_id={"zero": lax.rem(zero + s, zeros), "cols": col}, device_id_type=MESH))
            copies[-1].start()
    for s in range(1, zeros):
        copies.append(pltpu.make_async_remote_copy(
            src_ref=weight_ref, dst_ref=moved_refs[s - 1],
            send_sem=weight_send.at[s - 1], recv_sem=weight_recv.at[s - 1],
            device_id={"zero": lax.rem(zero + s, zeros), "cols": col}, device_id_type=MESH))
    for s in range(1, group):
        copy = pltpu.make_async_remote_copy(
            src_ref=mine, dst_ref=slots.at[me],
            send_sem=norm_send.at[s - 1], recv_sem=norm_recv.at[s - 1],
            device_id=device(lax.rem(me + s, group)), device_id_type=MESH)
        copy.start()
        copies.append(copy)
    for copy in copies[lows * (zeros - 1):(1 + lows) * (zeros - 1)]:
        copy.start()
    for k in range(lows):
        got_refs[k][0] = low_refs[k][...].T
    for copy in copies:
        copy.wait()
    for k in range(lows):
        for s in range(1, zeros):
            got_refs[k][s] = landed[k][s - 1].T
    slots[me] = mine[...]
    norm_ref[...] = jnp.concatenate([slots[g] for g in range(group)], axis=0).astype(norm_ref.dtype)


def exchange_first(zeros, cols, weight, train, step, lows):
    group = zeros * cols
    lanes = 128 if train.shape[0] % 128 == 0 else train.shape[0]
    tall = train.shape[0] // lanes
    outs = pl.pallas_call(
        functools.partial(first_kernel, zeros, cols, len(lows)),
        out_shape=[jax.ShapeDtypeStruct((group * tall, lanes), jnp.bfloat16)]
        + [jax.ShapeDtypeStruct((zeros,) + low.shape, low.dtype) for low in lows]
        + [jax.ShapeDtypeStruct(weight.shape, weight.dtype)] * (zeros - 1),
        in_specs=[pl.BlockSpec(memory_space=pl.ANY)] + [pl.BlockSpec(memory_space=pltpu.VMEM)] * (2 + len(lows)),
        out_specs=[pl.BlockSpec(memory_space=pltpu.VMEM)] * (1 + len(lows))
        + [pl.BlockSpec(memory_space=pl.ANY)] * (zeros - 1),
        scratch_shapes=[
            pltpu.VMEM((zeros - 1,) + low.shape[::-1], low.dtype) for low in lows
        ] + [
            pltpu.VMEM((tall, lanes), jnp.float32),
            pltpu.VMEM((group, tall, lanes), jnp.float32),
            pltpu.SemaphoreType.DMA((group - 1,)),
            pltpu.SemaphoreType.DMA((group - 1,)),
            pltpu.SemaphoreType.DMA((len(lows), zeros - 1)),
            pltpu.SemaphoreType.DMA((len(lows), zeros - 1)),
            pltpu.SemaphoreType.DMA((zeros - 1,)),
            pltpu.SemaphoreType.DMA((zeros - 1,)),
        ],
        cost_estimate=pl.CostEstimate(flops=0, bytes_accessed=2 ** 22, transcendentals=0),
        compiler_params=pltpu.CompilerParams(collective_id=0, has_side_effects=True),
    )(weight, train.reshape(tall, lanes), step.reshape(tall, lanes), *[low.T for low in lows])
    return outs[0].reshape(group * tall * lanes), outs[1:1 + len(lows)], outs[1 + len(lows):]


def merge_kernel(zeros, chunk, *refs):
    weight_refs = refs[:zeros]
    low_ref, high_ref, out_ref, column_ref, whole = refs[zeros:]
    zero = lax.axis_index("zero")
    rows, width = weight_refs[0].shape
    high = high_ref[...] * jnp.bfloat16(mix_rate)
    most = jnp.zeros((8, width), jnp.float32)
    for s in range(zeros):
        def step(i, most, s=s):
            at = pl.ds(pl.multiple_of(i * chunk, chunk), chunk)
            low = low_ref[s, at, :]
            value = weight_refs[s][at, :].astype(jnp.float32) + jnp.dot(
                low, high, preferred_element_type=jnp.float32)
            whole[s, at, :] = value
            return jnp.maximum(most, jnp.max(jnp.abs(value).reshape(chunk // 8, 8, width), axis=0))

        most = lax.fori_loop(0, rows // chunk, step, most, unroll=True)
    column = jnp.max(most, axis=0, keepdims=True)
    column_ref[...] = column
    scale = 1.0 / column
    for s in range(zeros):
        base = lax.rem(zero - s + zeros, zeros) * rows

        def put(i, carry, s=s, base=base):
            start = pl.multiple_of(i * chunk, chunk)
            out_ref[pl.ds(pl.multiple_of(base + start, chunk), chunk), :] = (
                whole[s, pl.ds(start, chunk), :] * scale).astype(out_ref.dtype)
            return carry

        lax.fori_loop(0, rows // chunk, put, 0, unroll=True)


def merge(zeros, weights, low, high):
    rows, columns = weights[0].shape
    rank = low.shape[2]
    width = min(512, columns)
    chunk = min(128, rows)
    serving, column = pl.pallas_call(
        functools.partial(merge_kernel, zeros, chunk),
        grid=(columns // width,),
        out_shape=[
            jax.ShapeDtypeStruct((rows * zeros, columns), jnp.bfloat16),
            jax.ShapeDtypeStruct((1, columns), jnp.float32),
        ],
        in_specs=[pl.BlockSpec((rows, width), lambda j: (0, j))] * zeros + [
            pl.BlockSpec((zeros, rows, rank), lambda j: (0, 0, 0)),
            pl.BlockSpec((rank, width), lambda j: (0, j)),
        ],
        out_specs=[
            pl.BlockSpec((rows * zeros, width), lambda j: (0, j)),
            pl.BlockSpec((1, width), lambda j: (0, j)),
        ],
        scratch_shapes=[pltpu.VMEM((zeros, rows, width), jnp.float32)],
        cost_estimate=pl.CostEstimate(
            flops=2 * rows * zeros * columns * rank,
            bytes_accessed=4 * rows * zeros * columns, transcendentals=0),
        compiler_params=pltpu.CompilerParams(dimension_semantics=("arbitrary",), vmem_limit_bytes=60 * 2 ** 20),
    )(*weights, low, high)
    return serving, column.reshape(columns)


def plain(zeros, cols, weight_gate, low_gate, high_gate, weight_up, low_up, high_up, norm_train, norm_step):
    def moved(array):
        return [array] + [
            lax.ppermute(array, "zero", [(i, (i + s) % zeros) for i in range(zeros)])
            for s in range(1, zeros)
        ]

    serve_norm, (all_gate, all_up), gates = exchange_first(
        zeros, cols, weight_gate, norm_train, norm_step, (low_gate, low_up))
    weight_up, all_up = lax.optimization_barrier((weight_up, all_up))
    ups = moved(weight_up)
    serving_gate, column_gate = merge(zeros, [weight_gate, *gates], all_gate, high_gate)
    serving_up, column_up = merge(zeros, ups, all_up, high_up)
    return (serving_gate, serving_up, column_gate, column_up, serve_norm)


def tile_values(raw_ref, low_ref, high, whole_ref, at, chunk):
    rows = raw_ref.shape[0]
    width = high.shape[1]

    def step(i, most):
        here = pl.ds(pl.multiple_of(i * chunk, chunk), chunk)
        value = raw_ref[here, at].astype(jnp.float32) + jnp.dot(
            low_ref[here, :], high, preferred_element_type=jnp.float32)
        whole_ref[here, at] = value
        return jnp.maximum(most, jnp.max(jnp.abs(value).reshape(chunk // 8, 8, width), axis=0))

    most = lax.fori_loop(0, rows // chunk, step, jnp.zeros((8, width), jnp.float32), unroll=True)
    return jnp.max(most, axis=0, keepdims=True)


def local_kernel(zeros, cols, width, chunk, gate_ref, up_ref, low_gate_ref, low_up_ref, high_gate_ref, high_up_ref,
                 train_ref, step_ref, whole_gate, whole_up, message, norm_ref,
                 raw, lows, lows_t, highs, mine, parts, weight_sems, small_sems, norm_sems, norm_send, norm_recv):
    zero, col = lax.axis_index("zero"), lax.axis_index("cols")
    me = zero * cols + col
    columns = raw.shape[2]
    pieces = columns // width
    ahead = 3

    barrier = pltpu.get_barrier_semaphore()
    for s in range(1, cols):
        for z in range(zeros):
            pl.semaphore_signal(barrier, inc=1, device_id={"zero": z, "cols": lax.rem(col + s, cols)}, device_id_type=MESH)

    loads = []
    for k, weight in enumerate((gate_ref, up_ref)):
        for j in range(pieces):
            at = pl.ds(j * width, width)
            loads.append(pltpu.make_async_copy(weight.at[:, at], raw.at[k, :, at], weight_sems.at[k, j]))
    small = []
    for k, (low, high) in enumerate(((low_gate_ref, high_gate_ref), (low_up_ref, high_up_ref))):
        small.append(pltpu.make_async_copy(low, lows_t.at[k], small_sems.at[k, 0]))
        small.append(pltpu.make_async_copy(high, highs.at[k], small_sems.at[k, 1]))
    norms = [pltpu.make_async_copy(ref, parts.at[i], norm_sems.at[i]) for i, ref in enumerate((train_ref, step_ref))]
    for copy in small[:2] + loads[:ahead] + norms + small[2:]:
        copy.start()

    def norm_copy(s, z, rank, recv):
        return pltpu.make_async_remote_copy(
            src_ref=mine, dst_ref=norm_ref.at[rank], send_sem=norm_send.at[s - 1, z], recv_sem=norm_recv.at[s - 1, recv],
            device_id={"zero": z, "cols": lax.rem(col + s, cols)}, device_id_type=MESH)

    for copy in norms:
        copy.wait()
    mine[...] = parts[0] + parts[1]
    norm_ref[me] = mine[...]
    norm_ref[(zeros - 1 - zero) * cols + col] = mine[...]
    tall, lanes = mine.shape
    for i in range(tall):
        message[:, pl.ds(2 * columns + i * lanes, lanes)] = mine[pl.ds(i, 1), :]
    entry = jnp.maximum(2 * pieces * (cols - 1 - col) // cols - 1, 0)
    for n in range(2 * pieces):
        @pl.when(entry == n)
        def _():
            pl.semaphore_wait(barrier, zeros * (cols - 1))
            for s in range(1, cols):
                for z in range(zeros):
                    norm_copy(s, z, me, zero).start()

        k, j = n // pieces, n % pieces
        if j == 0:
            small[2 * k].wait()
            small[2 * k + 1].wait()
            lows[k] = lows_t[k].T
        loads[n].wait()
        if n + ahead < len(loads):
            loads[n + ahead].start()
        at = pl.ds(j * width, width)
        high = highs[k, :, at] * jnp.bfloat16(mix_rate)
        message[:, pl.ds(k * columns + j * width, width)] = tile_values(
            raw.at[k], lows.at[k], high, (whole_gate, whole_up)[k], at, chunk)
    for s in range(1, cols):
        for z in range(zeros):
            norm_copy(s, z, me, zero).wait_send()
            norm_copy(s, z, z * cols + lax.rem(col - s + cols, cols), z).wait_recv()


def local_part(zeros, cols, gate, up, low_gate, low_up, high_gate, high_up, train, step):
    rows, columns = gate.shape
    rank = low_gate.shape[1]
    group = zeros * cols
    lanes = 128 if train.shape[0] % 128 == 0 else train.shape[0]
    tall = train.shape[0] // lanes
    width = min(512, columns)
    chunk = min(128, rows)
    dma = pltpu.SemaphoreType.DMA
    hbm, vmem = pl.BlockSpec(memory_space=pltpu.HBM), pl.BlockSpec(memory_space=pltpu.VMEM)
    return pl.pallas_call(
        functools.partial(local_kernel, zeros, cols, width, chunk),
        out_shape=[pltpu.VMEM((rows, columns), jnp.float32)] * 2
        + [pltpu.VMEM((1, 2 * columns + tall * lanes), jnp.float32), pltpu.VMEM((group, tall, lanes), jnp.float32)],
        in_specs=[hbm] * 8,
        out_specs=[vmem] * 4,
        scratch_shapes=[
            pltpu.VMEM((2, rows, columns), gate.dtype),
            pltpu.VMEM((2, rows, rank), gate.dtype),
            pltpu.VMEM((2, rank, rows), gate.dtype),
            pltpu.VMEM((2, rank, columns), gate.dtype),
            pltpu.VMEM((tall, lanes), jnp.float32),
            pltpu.VMEM((2, tall, lanes), jnp.float32),
            dma((2, columns // width)), dma((2, 2)), dma((2,)),
            dma((cols - 1, zeros)), dma((cols - 1, zeros)),
        ],
        cost_estimate=pl.CostEstimate(flops=2 ** 32, bytes_accessed=2 ** 23, transcendentals=0),
        compiler_params=pltpu.CompilerParams(collective_id=0, has_side_effects=True, vmem_limit_bytes=14 * 2 ** 20),
    )(*[pltpu.with_memory_space_constraint(array, pltpu.HBM) for array in (
        gate, up, low_gate.T, low_up.T, high_gate, high_up, train.reshape(tall, lanes), step.reshape(tall, lanes))])


def gate_kernel(zeros, width, chunk, whole, moved, low_gate_t, low_up_t, high_ref, message,
                out_ref, column_out, low_up, far_whole, stage, low_gate, column_ref, sems, column_sem):
    zero = lax.axis_index("zero")
    rows, columns = moved.shape
    copies = []
    low_gate[...] = low_gate_t[...].T
    for j in range(columns // width):
        at = pl.ds(j * width, width)
        column = jnp.maximum(message[:, at], tile_values(
            moved, low_gate, high_ref[:, at] * jnp.bfloat16(mix_rate), far_whole, at, chunk))
        column_ref[:, at] = column
        scale = 1.0 / column
        for k, (values, base) in enumerate(((whole, zero * rows), (far_whole, (zeros - 1 - zero) * rows))):
            for i in range(rows // chunk):
                here = pl.ds(i * chunk, chunk)
                stage[k, here, at] = (values[here, at] * scale).astype(stage.dtype)
            copies.append(pltpu.make_async_copy(
                stage.at[k, :, at], out_ref.at[pl.ds(pl.multiple_of(base, rows), rows), at], sems.at[k, j]))
            copies[-1].start()
    copies.append(pltpu.make_async_copy(column_ref, column_out, column_sem))
    copies[-1].start()
    low_up[...] = low_up_t[...].T
    for copy in copies:
        copy.wait()


def up_kernel(zeros, cols, chunk, whole, moved, low_up, high_ref, message, far_message, norm_in,
              out_ref, column_out, norm_out, stage, column_ref, slots, norm, sems, line_sems):
    zero, col = lax.axis_index("zero"), lax.axis_index("cols")
    rows, columns = moved.shape
    tall, lanes = norm_in.shape[1:]
    at = pl.ds(columns, columns)
    column = jnp.maximum(message[:, at], far_message[:, at])
    column_ref[...] = column
    scale = 1.0 / column
    high = high_ref[...] * jnp.bfloat16(mix_rate)
    copies = []
    for k, base in enumerate((zero * rows, (zeros - 1 - zero) * rows)):
        for i in range(rows // chunk):
            here = pl.ds(i * chunk, chunk)
            value = whole[here, :] if k == 0 else moved[here, :].astype(jnp.float32) + jnp.dot(
                low_up[here, :], high, preferred_element_type=jnp.float32)
            stage[k, here, :] = (value * scale).astype(stage.dtype)
            copies.append(pltpu.make_async_copy(
                stage.at[k, here, :], out_ref.at[pl.ds(pl.multiple_of(base + i * chunk, chunk), chunk), :], sems.at[k, i]))
            copies[-1].start()
        if k == 0:
            slots[...] = norm_in[...]
            for i in range(tall):
                slots[(zeros - 1 - zero) * cols + col, pl.ds(i, 1), :] = far_message[:, pl.ds(2 * columns + i * lanes, lanes)]
            norm[...] = jnp.concatenate([slots[g] for g in range(zeros * cols)], axis=0).astype(norm.dtype)
            for i, (src, dst) in enumerate(((column_ref, column_out), (norm, norm_out))):
                copies.append(pltpu.make_async_copy(src, dst, line_sems.at[i]))
                copies[-1].start()
    for copy in copies:
        copy.wait()


def per_device(zeros, cols, weight_gate, low_gate, high_gate, weight_up, low_up, high_up, norm_train, norm_step):
    if zeros != 2:
        return plain(zeros, cols, weight_gate, low_gate, high_gate, weight_up, low_up, high_up, norm_train, norm_step)
    rows, columns = weight_gate.shape
    rank = low_gate.shape[1]
    chunk = min(128, rows)
    width = min(512, columns)
    dma = pltpu.SemaphoreType.DMA

    def moved(array):
        return lax.ppermute(array, "zero", [(i, zeros - 1 - i) for i in range(zeros)])

    far_gate, far_low_gate = moved(weight_gate), moved(low_gate)
    far_low_up, far_up = moved(low_up), moved(weight_up)
    whole_gate, whole_up, message, norm = local_part(
        zeros, cols, weight_gate, weight_up, low_gate, low_up, high_gate, high_up, norm_train, norm_step)
    far_message = moved(message)
    hbm, vmem = pl.BlockSpec(memory_space=pltpu.HBM), pl.BlockSpec(memory_space=pltpu.VMEM)
    wide = jax.ShapeDtypeStruct((rows * zeros, columns), jnp.bfloat16)
    line = jax.ShapeDtypeStruct((1, columns), jnp.float32)
    group, tall, lanes = norm.shape
    serving_gate, column_gate, far_low = pl.pallas_call(
        functools.partial(gate_kernel, zeros, width, chunk),
        out_shape=[wide, line, pltpu.VMEM((rows, rank), low_up.dtype)],
        in_specs=[vmem] * 6,
        out_specs=[hbm] * 2 + [vmem],
        scratch_shapes=[pltpu.VMEM((rows, columns), jnp.float32), pltpu.VMEM((2, rows, columns), jnp.bfloat16),
                        pltpu.VMEM((rows, rank), low_gate.dtype), pltpu.VMEM((1, columns), jnp.float32),
                        dma((2, columns // width)), dma],
        cost_estimate=pl.CostEstimate(flops=2 ** 32, bytes_accessed=2 ** 23, transcendentals=0),
        compiler_params=pltpu.CompilerParams(vmem_limit_bytes=20 * 2 ** 20),
    )(whole_gate, far_gate, far_low_gate.T, far_low_up.T, high_gate, message)
    serving_up, column_up, serve_norm = pl.pallas_call(
        functools.partial(up_kernel, zeros, cols, chunk),
        out_shape=[wide, line, jax.ShapeDtypeStruct((group * tall, lanes), jnp.bfloat16)],
        in_specs=[vmem] * 7,
        out_specs=[hbm] * 3,
        scratch_shapes=[pltpu.VMEM((2, rows, columns), jnp.bfloat16), pltpu.VMEM((1, columns), jnp.float32),
                        pltpu.VMEM((group, tall, lanes), jnp.float32), pltpu.VMEM((group * tall, lanes), jnp.bfloat16),
                        dma((2, rows // chunk)), dma((2,))],
        cost_estimate=pl.CostEstimate(flops=2 ** 31, bytes_accessed=2 ** 23, transcendentals=0),
        compiler_params=pltpu.CompilerParams(vmem_limit_bytes=12 * 2 ** 20),
    )(whole_up, far_up, far_low, high_up, message, far_message, norm)
    return (serving_gate, serving_up, column_gate.reshape(columns), column_up.reshape(columns),
            serve_norm.reshape(group * tall * lanes))


def solution(mesh):
    in_specs = (
        P(("job", "zero"), "cols"),
        P(("job", "zero"), None),
        P("job", "cols"),
        P(("job", "zero"), "cols"),
        P(("job", "zero"), None),
        P("job", "cols"),
        P(("job", "zero", "cols")),
        P(("job", "zero", "cols")),
    )
    out_specs = (
        P("job", "cols"),
        P("job", "cols"),
        P(("job", "cols")),
        P(("job", "cols")),
        P("job"),
    )
    return jax.shard_map(
        functools.partial(per_device, mesh.shape["zero"], mesh.shape["cols"]),
        mesh=mesh, in_specs=in_specs, out_specs=out_specs, check_vma=False
    )
```

```python
import functools

import jax
import jax.numpy as jnp
from jax import lax
from jax.experimental import pallas as pl
from jax.experimental.pallas import tpu as pltpu
from jax.sharding import PartitionSpec as P


mix_rate = 2.0
MESH = pl.DeviceIdType.MESH


def first_kernel(zeros, cols, lows, weight_ref, *refs):
    train_ref, step_ref = refs[:2]
    low_refs = refs[2:2 + lows]
    norm_ref = refs[2 + lows]
    got_refs = refs[3 + lows:3 + 2 * lows]
    moved_refs = refs[3 + 2 * lows:2 + 2 * lows + zeros]
    refs = refs[2 + 2 * lows + zeros:]
    landed = refs[:lows]
    mine, slots, norm_send, norm_recv, low_send, low_recv, weight_send, weight_recv = refs[lows:]
    group = zeros * cols
    zero, col = lax.axis_index("zero"), lax.axis_index("cols")
    me = zero * cols + col

    def device(rank):
        return {"zero": rank // cols, "cols": lax.rem(rank, cols)}

    barrier = pltpu.get_barrier_semaphore()
    for s in range(1, group):
        pl.semaphore_signal(barrier, inc=1, device_id=device(lax.rem(me + s, group)), device_id_type=MESH)
    mine[...] = train_ref[...] + step_ref[...]
    pl.semaphore_wait(barrier, group - 1)

    copies = []
    for s in range(1, zeros):
        for k in range(lows):
            copies.append(pltpu.make_async_remote_copy(
                src_ref=low_refs[k], dst_ref=landed[k].at[s - 1],
                send_sem=low_send.at[k, s - 1], recv_sem=low_recv.at[k, s - 1],
                device_id={"zero": lax.rem(zero + s, zeros), "cols": col}, device_id_type=MESH))
            copies[-1].start()
    for s in range(1, zeros):
        copies.append(pltpu.make_async_remote_copy(
            src_ref=weight_ref, dst_ref=moved_refs[s - 1],
            send_sem=weight_send.at[s - 1], recv_sem=weight_recv.at[s - 1],
            device_id={"zero": lax.rem(zero + s, zeros), "cols": col}, device_id_type=MESH))
    for s in range(1, group):
        copy = pltpu.make_async_remote_copy(
            src_ref=mine, dst_ref=slots.at[me],
            send_sem=norm_send.at[s - 1], recv_sem=norm_recv.at[s - 1],
            device_id=device(lax.rem(me + s, group)), device_id_type=MESH)
        copy.start()
        copies.append(copy)
    for copy in copies[lows * (zeros - 1):(1 + lows) * (zeros - 1)]:
        copy.start()
    for k in range(lows):
        got_refs[k][0] = low_refs[k][...].T
    for copy in copies:
        copy.wait()
    for k in range(lows):
        for s in range(1, zeros):
            got_refs[k][s] = landed[k][s - 1].T
    slots[me] = mine[...]
    norm_ref[...] = jnp.concatenate([slots[g] for g in range(group)], axis=0).astype(norm_ref.dtype)


def exchange_first(zeros, cols, weight, train, step, lows):
    group = zeros * cols
    lanes = 128 if train.shape[0] % 128 == 0 else train.shape[0]
    tall = train.shape[0] // lanes
    outs = pl.pallas_call(
        functools.partial(first_kernel, zeros, cols, len(lows)),
        out_shape=[jax.ShapeDtypeStruct((group * tall, lanes), jnp.bfloat16)]
        + [jax.ShapeDtypeStruct((zeros,) + low.shape, low.dtype) for low in lows]
        + [jax.ShapeDtypeStruct(weight.shape, weight.dtype)] * (zeros - 1),
        in_specs=[pl.BlockSpec(memory_space=pl.ANY)] + [pl.BlockSpec(memory_space=pltpu.VMEM)] * (2 + len(lows)),
        out_specs=[pl.BlockSpec(memory_space=pltpu.VMEM)] * (1 + len(lows))
        + [pl.BlockSpec(memory_space=pl.ANY)] * (zeros - 1),
        scratch_shapes=[
            pltpu.VMEM((zeros - 1,) + low.shape[::-1], low.dtype) for low in lows
        ] + [
            pltpu.VMEM((tall, lanes), jnp.float32),
            pltpu.VMEM((group, tall, lanes), jnp.float32),
            pltpu.SemaphoreType.DMA((group - 1,)),
            pltpu.SemaphoreType.DMA((group - 1,)),
            pltpu.SemaphoreType.DMA((len(lows), zeros - 1)),
            pltpu.SemaphoreType.DMA((len(lows), zeros - 1)),
            pltpu.SemaphoreType.DMA((zeros - 1,)),
            pltpu.SemaphoreType.DMA((zeros - 1,)),
        ],
        cost_estimate=pl.CostEstimate(flops=0, bytes_accessed=2 ** 22, transcendentals=0),
        compiler_params=pltpu.CompilerParams(collective_id=0, has_side_effects=True),
    )(weight, train.reshape(tall, lanes), step.reshape(tall, lanes), *[low.T for low in lows])
    return outs[0].reshape(group * tall * lanes), outs[1:1 + len(lows)], outs[1 + len(lows):]


def merge_kernel(zeros, chunk, *refs):
    weight_refs = refs[:zeros]
    low_ref, high_ref, out_ref, column_ref, whole = refs[zeros:]
    zero = lax.axis_index("zero")
    rows, width = weight_refs[0].shape
    high = high_ref[...] * jnp.bfloat16(mix_rate)
    most = jnp.zeros((8, width), jnp.float32)
    for s in range(zeros):
        def step(i, most, s=s):
            at = pl.ds(pl.multiple_of(i * chunk, chunk), chunk)
            low = low_ref[s, at, :]
            value = weight_refs[s][at, :].astype(jnp.float32) + jnp.dot(
                low, high, preferred_element_type=jnp.float32)
            whole[s, at, :] = value
            return jnp.maximum(most, jnp.max(jnp.abs(value).reshape(chunk // 8, 8, width), axis=0))

        most = lax.fori_loop(0, rows // chunk, step, most, unroll=True)
    column = jnp.max(most, axis=0, keepdims=True)
    column_ref[...] = column
    scale = 1.0 / column
    for s in range(zeros):
        base = lax.rem(zero - s + zeros, zeros) * rows

        def put(i, carry, s=s, base=base):
            start = pl.multiple_of(i * chunk, chunk)
            out_ref[pl.ds(pl.multiple_of(base + start, chunk), chunk), :] = (
                whole[s, pl.ds(start, chunk), :] * scale).astype(out_ref.dtype)
            return carry

        lax.fori_loop(0, rows // chunk, put, 0, unroll=True)


def merge(zeros, weights, low, high):
    rows, columns = weights[0].shape
    rank = low.shape[2]
    width = min(512, columns)
    chunk = min(128, rows)
    serving, column = pl.pallas_call(
        functools.partial(merge_kernel, zeros, chunk),
        grid=(columns // width,),
        out_shape=[
            jax.ShapeDtypeStruct((rows * zeros, columns), jnp.bfloat16),
            jax.ShapeDtypeStruct((1, columns), jnp.float32),
        ],
        in_specs=[pl.BlockSpec((rows, width), lambda j: (0, j))] * zeros + [
            pl.BlockSpec((zeros, rows, rank), lambda j: (0, 0, 0)),
            pl.BlockSpec((rank, width), lambda j: (0, j)),
        ],
        out_specs=[
            pl.BlockSpec((rows * zeros, width), lambda j: (0, j)),
            pl.BlockSpec((1, width), lambda j: (0, j)),
        ],
        scratch_shapes=[pltpu.VMEM((zeros, rows, width), jnp.float32)],
        cost_estimate=pl.CostEstimate(
            flops=2 * rows * zeros * columns * rank,
            bytes_accessed=4 * rows * zeros * columns, transcendentals=0),
        compiler_params=pltpu.CompilerParams(dimension_semantics=("arbitrary",), vmem_limit_bytes=60 * 2 ** 20),
    )(*weights, low, high)
    return serving, column.reshape(columns)


def plain(zeros, cols, weight_gate, low_gate, high_gate, weight_up, low_up, high_up, norm_train, norm_step):
    def moved(array):
        return [array] + [
            lax.ppermute(array, "zero", [(i, (i + s) % zeros) for i in range(zeros)])
            for s in range(1, zeros)
        ]

    serve_norm, (all_gate, all_up), gates = exchange_first(
        zeros, cols, weight_gate, norm_train, norm_step, (low_gate, low_up))
    weight_up, all_up = lax.optimization_barrier((weight_up, all_up))
    ups = moved(weight_up)
    serving_gate, column_gate = merge(zeros, [weight_gate, *gates], all_gate, high_gate)
    serving_up, column_up = merge(zeros, ups, all_up, high_up)
    return (serving_gate, serving_up, column_gate, column_up, serve_norm)


def local_kernel(zeros, cols, width, chunk, gate_ref, up_ref, low_gate_ref, low_up_ref, high_gate_ref, high_up_ref,
                 train_ref, step_ref, whole_gate, whole_up, up_first, up_second, far_lows, most, far_most, norm_ref,
                 raw, lows, lows_t, highs, parts, weight_sems, small_sems, norm_sems, norm_send, norm_recv,
                 near_send, near_recv):
    zero, col = lax.axis_index("zero"), lax.axis_index("cols")
    me = zero * cols + col
    rows, columns = raw.shape
    pieces = columns // width
    split = up_first.shape[0]
    ahead = 3

    barrier = pltpu.get_barrier_semaphore()
    for z in range(1, zeros):
        pl.semaphore_signal(barrier, inc=1, device_id={"zero": lax.rem(zero + z, zeros), "cols": col}, device_id_type=MESH)
    for s in range(1, cols):
        for z in range(zeros):
            pl.semaphore_signal(barrier, inc=1, device_id={"zero": z, "cols": lax.rem(col + s, cols)}, device_id_type=MESH)

    loads = []
    for j in range(pieces):
        at = pl.ds(j * width, width)
        loads.append([pltpu.make_async_copy(gate_ref.at[:, at], raw.at[:, at], weight_sems.at[0, j])])
    for j in range(pieces):
        at = pl.ds(j * width, width)
        loads.append([pltpu.make_async_copy(up_ref.at[pl.ds(0, split), at], up_first.at[:, at], weight_sems.at[1, j]),
                      pltpu.make_async_copy(up_ref.at[pl.ds(split, rows - split), at], up_second.at[:, at], weight_sems.at[2, j])])
    small = []
    for k, (low, high) in enumerate(((low_gate_ref, high_gate_ref), (low_up_ref, high_up_ref))):
        small.append(pltpu.make_async_copy(low, lows_t.at[k], small_sems.at[k, 0]))
        small.append(pltpu.make_async_copy(high, highs.at[k], small_sems.at[k, 1]))
    norms = [pltpu.make_async_copy(ref, parts.at[i], norm_sems.at[i]) for i, ref in enumerate((train_ref, step_ref))]
    for copy in norms + small[:2] + sum(loads[:ahead], []) + small[2:]:
        copy.start()

    def norm_copy(i, s, z, rank, recv):
        return pltpu.make_async_remote_copy(
            src_ref=(train_ref, step_ref)[i], dst_ref=norm_ref.at[i, rank],
            send_sem=norm_send.at[i, s - 1, z], recv_sem=norm_recv.at[i, s - 1, recv],
            device_id={"zero": z, "cols": lax.rem(col + s, cols)}, device_id_type=MESH)

    def near_copy(i, src, dst):
        return pltpu.make_async_remote_copy(
            src_ref=src, dst_ref=dst, send_sem=near_send.at[i], recv_sem=near_recv.at[i],
            device_id={"zero": zeros - 1 - zero, "cols": col}, device_id_type=MESH)

    def near_copies(rank):
        return [near_copy(0, low_gate_ref, far_lows.at[0]), near_copy(1, low_up_ref, far_lows.at[1]),
                near_copy(2, train_ref, norm_ref.at[0, rank]), near_copy(3, step_ref, norm_ref.at[1, rank])]

    peers = [(i, s, z) for s in range(cols - 1, 0, -1) for z in range(zeros) for i in range(2)]
    entry = jnp.maximum(2 * pieces * (cols - 1 - col) // cols - 1, 0)
    for n in range(2 * pieces):
        @pl.when(entry == n)
        def _():
            pl.semaphore_wait(barrier, zeros * cols - 1)
            for i, s, z in peers:
                norm_copy(i, s, z, me, zero).start()
            for copy in near_copies(me):
                copy.start()

        k, j = n // pieces, n % pieces
        if j == 0:
            small[2 * k].wait()
            small[2 * k + 1].wait()
            lows[k] = lows_t[k].T
        for copy in loads[n]:
            copy.wait()
        if n + ahead < len(loads):
            for copy in loads[n + ahead]:
                copy.start()
        at = pl.ds(j * width, width)
        high = highs[k, :, at] * jnp.bfloat16(mix_rate)
        whole = (whole_gate, whole_up)[k]
        value_most = jnp.zeros((8, width), jnp.float32)
        for i in range(rows // chunk):
            here = pl.ds(i * chunk, chunk)
            if k == 0:
                part = raw[here, at]
            elif i * chunk < split:
                part = up_first[here, at]
            else:
                part = up_second[pl.ds(i * chunk - split, chunk), at]
            value = part.astype(jnp.float32) + jnp.dot(lows[k, here, :], high, preferred_element_type=jnp.float32)
            whole[here, at] = value
            value_most = jnp.maximum(value_most, jnp.max(jnp.abs(value).reshape(chunk // 8, 8, width), axis=0))
        most[:, pl.ds(k * columns + j * width, width)] = jnp.max(value_most, axis=0, keepdims=True)
    give = near_copy(4, most, far_most)
    give.start()
    for copy in norms:
        copy.wait()
    for i in range(2):
        norm_ref[i, me] = parts[i]
    for i, s, z in peers:
        norm_copy(i, s, z, me, zero).wait_send()
        norm_copy(i, s, z, z * cols + lax.rem(col - s + cols, cols), z).wait_recv()
    for copy in near_copies(me):
        copy.wait_send()
    for copy in near_copies((zeros - 1 - zero) * cols + col):
        copy.wait_recv()
    give.wait()


def local_part(zeros, cols, split, gate, up, low_gate, low_up, high_gate, high_up, train, step):
    rows, columns = gate.shape
    rank = low_gate.shape[1]
    group = zeros * cols
    lanes = 128 if train.shape[0] % 128 == 0 else train.shape[0]
    tall = train.shape[0] // lanes
    width = min(512, columns)
    chunk = min(128, rows)
    dma = pltpu.SemaphoreType.DMA
    hbm, vmem = pl.BlockSpec(memory_space=pltpu.HBM), pl.BlockSpec(memory_space=pltpu.VMEM)
    return pl.pallas_call(
        functools.partial(local_kernel, zeros, cols, width, chunk),
        out_shape=[pltpu.VMEM((rows, columns), jnp.float32)] * 2
        + [pltpu.VMEM((split, columns), up.dtype), pltpu.VMEM((rows - split, columns), up.dtype),
           pltpu.VMEM((2, rank, rows), gate.dtype)]
        + [pltpu.VMEM((1, 2 * columns), jnp.float32)] * 2
        + [pltpu.VMEM((2, group, tall, lanes), jnp.float32)],
        in_specs=[hbm] * 8,
        out_specs=[vmem] * 8,
        scratch_shapes=[
            pltpu.VMEM((rows, columns), gate.dtype),
            pltpu.VMEM((2, rows, rank), gate.dtype),
            pltpu.VMEM((2, rank, rows), gate.dtype),
            pltpu.VMEM((2, rank, columns), gate.dtype),
            pltpu.VMEM((2, tall, lanes), jnp.float32),
            dma((3, columns // width)), dma((2, 2)), dma((2,)),
            dma((2, cols - 1, zeros)), dma((2, cols - 1, zeros)), dma((5,)), dma((5,)),
        ],
        cost_estimate=pl.CostEstimate(flops=2 ** 32, bytes_accessed=2 ** 23, transcendentals=0),
        compiler_params=pltpu.CompilerParams(collective_id=0, has_side_effects=True, vmem_limit_bytes=10 * 2 ** 20),
    )(*[pltpu.with_memory_space_constraint(array, pltpu.HBM) for array in (
        gate, up, low_gate.T, low_up.T, high_gate, high_up, train.reshape(tall, lanes), step.reshape(tall, lanes))])


def write_rows(value_of, chunk, stage, out_ref, base, sems):
    copies = []
    for i in range(stage.shape[0] // chunk):
        here = pl.ds(i * chunk, chunk)
        stage[here, :] = value_of(here).astype(stage.dtype)
        copies.append(pltpu.make_async_copy(
            stage.at[here, :], out_ref.at[pl.ds(pl.multiple_of(base + i * chunk, chunk), chunk), :], sems.at[i]))
        copies[-1].start()
    return copies


def far_value(moved, low_ref, first, high, scale):
    return lambda here: (moved[here, :].astype(jnp.float32) + jnp.dot(
        low_ref[pl.ds(first + here.start, here.size), :], high, preferred_element_type=jnp.float32)) * scale


def most_kernel(zeros, cols, chunk, whole_gate, whole_up, moved, far_lows, high_ref, most, far_most, norm_in,
                gate_out, up_out, column_gate_out, column_up_out, norm_out, low_up, column_up,
                stage, low_gate, column_gate, norm, sems, line_sems):
    zero = lax.axis_index("zero")
    rows, columns = moved.shape
    near, far = zero * rows, (zeros - 1 - zero) * rows
    for k, column in enumerate((column_gate, column_up)):
        at = pl.ds(k * columns, columns)
        column[...] = jnp.maximum(most[:, at], far_most[:, at])
    scale = 1.0 / column_up[...]
    copies = write_rows(lambda here: whole_up[here, :] * scale, chunk, stage.at[0], up_out, near, sems.at[0])
    gate_scale = 1.0 / column_gate[...]
    copies += write_rows(lambda here: whole_gate[here, :] * gate_scale, chunk, stage.at[1], gate_out, near, sems.at[1])
    norm[...] = jnp.concatenate([norm_in[0, g] + norm_in[1, g] for g in range(zeros * cols)], axis=0).astype(norm.dtype)
    for i, (src, dst) in enumerate(((column_gate, column_gate_out), (column_up, column_up_out), (norm, norm_out))):
        copies.append(pltpu.make_async_copy(src, dst, line_sems.at[i]))
        copies[-1].start()
    low_gate[...] = far_lows[0].T
    high = high_ref[...] * jnp.bfloat16(mix_rate)
    copies += write_rows(far_value(moved, low_gate, 0, high, gate_scale), chunk, stage.at[2], gate_out, far, sems.at[2])
    low_up[...] = far_lows[1].T
    for copy in copies:
        copy.wait()


def last_kernel(zeros, chunk, rows, first, moved, low_ref, high_ref, column_ref, up_in, up_out, stage, sems):
    zero = lax.axis_index("zero")
    high, scale = high_ref[...] * jnp.bfloat16(mix_rate), 1.0 / column_ref[...]
    for copy in write_rows(far_value(moved, low_ref, first, high, scale), chunk, stage, up_out,
                           (zeros - 1 - zero) * rows + first, sems):
        copy.wait()


def per_device(zeros, cols, weight_gate, low_gate, high_gate, weight_up, low_up, high_up, norm_train, norm_step):
    rows, columns = weight_gate.shape
    rank = low_gate.shape[1]
    chunk = min(128, rows)
    split = rows * 3 // 4 // chunk * chunk
    if zeros != 2 or not split:
        return plain(zeros, cols, weight_gate, low_gate, high_gate, weight_up, low_up, high_up, norm_train, norm_step)

    def moved(array):
        return lax.ppermute(array, "zero", [(i, zeros - 1 - i) for i in range(zeros)])

    far_gate = moved(weight_gate)
    whole_gate, whole_up, up_first, up_second, far_lows, most, far_most, norm = local_part(
        zeros, cols, split, weight_gate, weight_up, low_gate, low_up, high_gate, high_up, norm_train, norm_step)
    far_up = [moved(up_first), moved(up_second)]
    hbm, vmem = pl.BlockSpec(memory_space=pltpu.HBM), pl.BlockSpec(memory_space=pltpu.VMEM)
    wide = jax.ShapeDtypeStruct((rows * zeros, columns), jnp.bfloat16)
    line = jax.ShapeDtypeStruct((1, columns), jnp.float32)
    group, tall, lanes = norm.shape[1:]
    serving_gate, serving_up, column_gate, column_up, serve_norm, far_low, up_line = pl.pallas_call(
        functools.partial(most_kernel, zeros, cols, chunk),
        out_shape=[wide, wide, line, line, jax.ShapeDtypeStruct((group * tall, lanes), jnp.bfloat16),
                   pltpu.VMEM((rows, rank), low_up.dtype), pltpu.VMEM((1, columns), jnp.float32)],
        in_specs=[vmem] * 8,
        out_specs=[hbm] * 5 + [vmem] * 2,
        scratch_shapes=[pltpu.VMEM((3, rows, columns), jnp.bfloat16), pltpu.VMEM((rows, rank), low_gate.dtype),
                        pltpu.VMEM((1, columns), jnp.float32), pltpu.VMEM((group * tall, lanes), jnp.bfloat16),
                        pltpu.SemaphoreType.DMA((3, rows // chunk)), pltpu.SemaphoreType.DMA((3,))],
        cost_estimate=pl.CostEstimate(flops=2 ** 32, bytes_accessed=3 * 2 ** 22, transcendentals=0),
        compiler_params=pltpu.CompilerParams(vmem_limit_bytes=16 * 2 ** 20),
    )(whole_gate, whole_up, far_gate, far_lows, high_gate, most, far_most, norm)
    for far, first in zip(far_up, (0, split)):
        serving_up = pl.pallas_call(
            functools.partial(last_kernel, zeros, chunk, rows, first),
            out_shape=wide,
            in_specs=[vmem] * 4 + [hbm],
            out_specs=hbm,
            input_output_aliases={4: 0},
            scratch_shapes=[pltpu.VMEM(far.shape, jnp.bfloat16), pltpu.SemaphoreType.DMA((far.shape[0] // chunk,))],
            cost_estimate=pl.CostEstimate(flops=2 ** 30, bytes_accessed=2 ** 22, transcendentals=0),
            compiler_params=pltpu.CompilerParams(vmem_limit_bytes=16 * 2 ** 20),
        )(far, far_low, high_up, up_line, serving_up)
    return (serving_gate, serving_up, column_gate.reshape(columns), column_up.reshape(columns),
            serve_norm.reshape(group * tall * lanes))


def solution(mesh):
    in_specs = (
        P(("job", "zero"), "cols"),
        P(("job", "zero"), None),
        P("job", "cols"),
        P(("job", "zero"), "cols"),
        P(("job", "zero"), None),
        P("job", "cols"),
        P(("job", "zero", "cols")),
        P(("job", "zero", "cols")),
    )
    out_specs = (
        P("job", "cols"),
        P("job", "cols"),
        P(("job", "cols")),
        P(("job", "cols")),
        P("job"),
    )
    return jax.shard_map(
        functools.partial(per_device, mesh.shape["zero"], mesh.shape["cols"]),
        mesh=mesh, in_specs=in_specs, out_specs=out_specs, check_vma=False
    )
```

```python
import functools

import jax
import jax.numpy as jnp
from jax import lax
from jax.experimental import pallas as pl
from jax.experimental.pallas import tpu as pltpu
from jax.sharding import PartitionSpec as P


mix_rate = 2.0
MESH = pl.DeviceIdType.MESH


def first_kernel(zeros, cols, lows, weight_ref, *refs):
    train_ref, step_ref = refs[:2]
    low_refs = refs[2:2 + lows]
    norm_ref = refs[2 + lows]
    got_refs = refs[3 + lows:3 + 2 * lows]
    moved_refs = refs[3 + 2 * lows:2 + 2 * lows + zeros]
    refs = refs[2 + 2 * lows + zeros:]
    landed = refs[:lows]
    mine, slots, norm_send, norm_recv, low_send, low_recv, weight_send, weight_recv = refs[lows:]
    group = zeros * cols
    zero, col = lax.axis_index("zero"), lax.axis_index("cols")
    me = zero * cols + col

    def device(rank):
        return {"zero": rank // cols, "cols": lax.rem(rank, cols)}

    barrier = pltpu.get_barrier_semaphore()
    for s in range(1, group):
        pl.semaphore_signal(barrier, inc=1, device_id=device(lax.rem(me + s, group)), device_id_type=MESH)
    mine[...] = train_ref[...] + step_ref[...]
    pl.semaphore_wait(barrier, group - 1)

    copies = []
    for s in range(1, zeros):
        for k in range(lows):
            copies.append(pltpu.make_async_remote_copy(
                src_ref=low_refs[k], dst_ref=landed[k].at[s - 1],
                send_sem=low_send.at[k, s - 1], recv_sem=low_recv.at[k, s - 1],
                device_id={"zero": lax.rem(zero + s, zeros), "cols": col}, device_id_type=MESH))
            copies[-1].start()
    for s in range(1, zeros):
        copies.append(pltpu.make_async_remote_copy(
            src_ref=weight_ref, dst_ref=moved_refs[s - 1],
            send_sem=weight_send.at[s - 1], recv_sem=weight_recv.at[s - 1],
            device_id={"zero": lax.rem(zero + s, zeros), "cols": col}, device_id_type=MESH))
    for s in range(1, group):
        copy = pltpu.make_async_remote_copy(
            src_ref=mine, dst_ref=slots.at[me],
            send_sem=norm_send.at[s - 1], recv_sem=norm_recv.at[s - 1],
            device_id=device(lax.rem(me + s, group)), device_id_type=MESH)
        copy.start()
        copies.append(copy)
    for copy in copies[lows * (zeros - 1):(1 + lows) * (zeros - 1)]:
        copy.start()
    for k in range(lows):
        got_refs[k][0] = low_refs[k][...].T
    for copy in copies:
        copy.wait()
    for k in range(lows):
        for s in range(1, zeros):
            got_refs[k][s] = landed[k][s - 1].T
    slots[me] = mine[...]
    norm_ref[...] = jnp.concatenate([slots[g] for g in range(group)], axis=0).astype(norm_ref.dtype)


def exchange_first(zeros, cols, weight, train, step, lows):
    group = zeros * cols
    lanes = 128 if train.shape[0] % 128 == 0 else train.shape[0]
    tall = train.shape[0] // lanes
    outs = pl.pallas_call(
        functools.partial(first_kernel, zeros, cols, len(lows)),
        out_shape=[jax.ShapeDtypeStruct((group * tall, lanes), jnp.bfloat16)]
        + [jax.ShapeDtypeStruct((zeros,) + low.shape, low.dtype) for low in lows]
        + [jax.ShapeDtypeStruct(weight.shape, weight.dtype)] * (zeros - 1),
        in_specs=[pl.BlockSpec(memory_space=pl.ANY)] + [pl.BlockSpec(memory_space=pltpu.VMEM)] * (2 + len(lows)),
        out_specs=[pl.BlockSpec(memory_space=pltpu.VMEM)] * (1 + len(lows))
        + [pl.BlockSpec(memory_space=pl.ANY)] * (zeros - 1),
        scratch_shapes=[
            pltpu.VMEM((zeros - 1,) + low.shape[::-1], low.dtype) for low in lows
        ] + [
            pltpu.VMEM((tall, lanes), jnp.float32),
            pltpu.VMEM((group, tall, lanes), jnp.float32),
            pltpu.SemaphoreType.DMA((group - 1,)),
            pltpu.SemaphoreType.DMA((group - 1,)),
            pltpu.SemaphoreType.DMA((len(lows), zeros - 1)),
            pltpu.SemaphoreType.DMA((len(lows), zeros - 1)),
            pltpu.SemaphoreType.DMA((zeros - 1,)),
            pltpu.SemaphoreType.DMA((zeros - 1,)),
        ],
        cost_estimate=pl.CostEstimate(flops=0, bytes_accessed=2 ** 22, transcendentals=0),
        compiler_params=pltpu.CompilerParams(collective_id=0, has_side_effects=True),
    )(weight, train.reshape(tall, lanes), step.reshape(tall, lanes), *[low.T for low in lows])
    return outs[0].reshape(group * tall * lanes), outs[1:1 + len(lows)], outs[1 + len(lows):]


def merge_kernel(zeros, chunk, *refs):
    weight_refs = refs[:zeros]
    low_ref, high_ref, out_ref, column_ref, whole = refs[zeros:]
    zero = lax.axis_index("zero")
    rows, width = weight_refs[0].shape
    high = high_ref[...] * jnp.bfloat16(mix_rate)
    most = jnp.zeros((8, width), jnp.float32)
    for s in range(zeros):
        def step(i, most, s=s):
            at = pl.ds(pl.multiple_of(i * chunk, chunk), chunk)
            low = low_ref[s, at, :]
            value = weight_refs[s][at, :].astype(jnp.float32) + jnp.dot(
                low, high, preferred_element_type=jnp.float32)
            whole[s, at, :] = value
            return jnp.maximum(most, jnp.max(jnp.abs(value).reshape(chunk // 8, 8, width), axis=0))

        most = lax.fori_loop(0, rows // chunk, step, most, unroll=True)
    column = jnp.max(most, axis=0, keepdims=True)
    column_ref[...] = column
    scale = 1.0 / column
    for s in range(zeros):
        base = lax.rem(zero - s + zeros, zeros) * rows

        def put(i, carry, s=s, base=base):
            start = pl.multiple_of(i * chunk, chunk)
            out_ref[pl.ds(pl.multiple_of(base + start, chunk), chunk), :] = (
                whole[s, pl.ds(start, chunk), :] * scale).astype(out_ref.dtype)
            return carry

        lax.fori_loop(0, rows // chunk, put, 0, unroll=True)


def merge(zeros, weights, low, high):
    rows, columns = weights[0].shape
    rank = low.shape[2]
    width = min(512, columns)
    chunk = min(128, rows)
    serving, column = pl.pallas_call(
        functools.partial(merge_kernel, zeros, chunk),
        grid=(columns // width,),
        out_shape=[
            jax.ShapeDtypeStruct((rows * zeros, columns), jnp.bfloat16),
            jax.ShapeDtypeStruct((1, columns), jnp.float32),
        ],
        in_specs=[pl.BlockSpec((rows, width), lambda j: (0, j))] * zeros + [
            pl.BlockSpec((zeros, rows, rank), lambda j: (0, 0, 0)),
            pl.BlockSpec((rank, width), lambda j: (0, j)),
        ],
        out_specs=[
            pl.BlockSpec((rows * zeros, width), lambda j: (0, j)),
            pl.BlockSpec((1, width), lambda j: (0, j)),
        ],
        scratch_shapes=[pltpu.VMEM((zeros, rows, width), jnp.float32)],
        cost_estimate=pl.CostEstimate(
            flops=2 * rows * zeros * columns * rank,
            bytes_accessed=4 * rows * zeros * columns, transcendentals=0),
        compiler_params=pltpu.CompilerParams(dimension_semantics=("arbitrary",), vmem_limit_bytes=60 * 2 ** 20),
    )(*weights, low, high)
    return serving, column.reshape(columns)


def plain(zeros, cols, weight_gate, low_gate, high_gate, weight_up, low_up, high_up, norm_train, norm_step):
    def moved(array):
        return [array] + [
            lax.ppermute(array, "zero", [(i, (i + s) % zeros) for i in range(zeros)])
            for s in range(1, zeros)
        ]

    serve_norm, (all_gate, all_up), gates = exchange_first(
        zeros, cols, weight_gate, norm_train, norm_step, (low_gate, low_up))
    weight_up, all_up = lax.optimization_barrier((weight_up, all_up))
    ups = moved(weight_up)
    serving_gate, column_gate = merge(zeros, [weight_gate, *gates], all_gate, high_gate)
    serving_up, column_up = merge(zeros, ups, all_up, high_up)
    return (serving_gate, serving_up, column_gate, column_up, serve_norm)


def local_kernel(zeros, cols, width, chunk, gate_ref, up_ref, low_gate_ref, low_up_ref, high_gate_ref, high_up_ref,
                 train_ref, step_ref, whole_gate, whole_up, up_first, up_second, far_lows, most, far_most, norm_ref,
                 raw, lows, lows_t, highs, parts, weight_sems, small_sems, norm_sems, norm_send, norm_recv,
                 near_send, near_recv):
    zero, col = lax.axis_index("zero"), lax.axis_index("cols")
    me = zero * cols + col
    rows, columns = raw.shape
    pieces = columns // width
    split = up_first.shape[0]
    ahead = 3

    barrier = pltpu.get_barrier_semaphore()
    for z in range(1, zeros):
        pl.semaphore_signal(barrier, inc=1, device_id={"zero": lax.rem(zero + z, zeros), "cols": col}, device_id_type=MESH)
    for s in range(1, cols):
        for z in range(zeros):
            pl.semaphore_signal(barrier, inc=1, device_id={"zero": z, "cols": lax.rem(col + s, cols)}, device_id_type=MESH)

    loads = []
    for j in range(pieces):
        at = pl.ds(j * width, width)
        loads.append([pltpu.make_async_copy(gate_ref.at[:, at], raw.at[:, at], weight_sems.at[0, j])])
    for j in range(pieces):
        at = pl.ds(j * width, width)
        loads.append([pltpu.make_async_copy(up_ref.at[pl.ds(0, split), at], up_first.at[:, at], weight_sems.at[1, j]),
                      pltpu.make_async_copy(up_ref.at[pl.ds(split, rows - split), at], up_second.at[:, at], weight_sems.at[2, j])])
    small = []
    for k, (low, high) in enumerate(((low_gate_ref, high_gate_ref), (low_up_ref, high_up_ref))):
        small.append(pltpu.make_async_copy(low, lows_t.at[k], small_sems.at[k, 0]))
        small.append(pltpu.make_async_copy(high, highs.at[k], small_sems.at[k, 1]))
    norms = [pltpu.make_async_copy(ref, parts.at[i], norm_sems.at[i]) for i, ref in enumerate((train_ref, step_ref))]
    for copy in norms + small[:2] + sum(loads[:ahead], []) + small[2:]:
        copy.start()

    def norm_copy(i, s, z, rank, recv):
        return pltpu.make_async_remote_copy(
            src_ref=(train_ref, step_ref)[i], dst_ref=norm_ref.at[i, rank],
            send_sem=norm_send.at[i, s - 1, z], recv_sem=norm_recv.at[i, s - 1, recv],
            device_id={"zero": z, "cols": lax.rem(col + s, cols)}, device_id_type=MESH)

    def near_copy(i, src, dst):
        return pltpu.make_async_remote_copy(
            src_ref=src, dst_ref=dst, send_sem=near_send.at[i], recv_sem=near_recv.at[i],
            device_id={"zero": zeros - 1 - zero, "cols": col}, device_id_type=MESH)

    def near_copies(rank):
        return [near_copy(0, low_gate_ref, far_lows.at[0]), near_copy(1, low_up_ref, far_lows.at[1]),
                near_copy(2, train_ref, norm_ref.at[0, rank]), near_copy(3, step_ref, norm_ref.at[1, rank])]

    peers = [(i, s, z) for s in range(cols - 1, 0, -1) for z in range(zeros) for i in range(2)]
    entry = jnp.maximum(2 * pieces * (cols - 1 - col) // cols - 1, 0)
    for n in range(2 * pieces):
        @pl.when(entry == n)
        def _():
            pl.semaphore_wait(barrier, zeros * cols - 1)
            for i, s, z in peers:
                norm_copy(i, s, z, me, zero).start()
            for copy in near_copies(me):
                copy.start()

        k, j = n // pieces, n % pieces
        if j == 0:
            small[2 * k].wait()
            small[2 * k + 1].wait()
            lows[k] = lows_t[k].T
        for copy in loads[n]:
            copy.wait()
        if n + ahead < len(loads):
            for copy in loads[n + ahead]:
                copy.start()
        at = pl.ds(j * width, width)
        high = highs[k, :, at] * jnp.bfloat16(mix_rate)
        whole = (whole_gate, whole_up)[k]
        value_most = jnp.zeros((8, width), jnp.float32)
        for i in range(rows // chunk):
            here = pl.ds(i * chunk, chunk)
            if k == 0:
                part = raw[here, at]
            elif i * chunk < split:
                part = up_first[here, at]
            else:
                part = up_second[pl.ds(i * chunk - split, chunk), at]
            value = part.astype(jnp.float32) + jnp.dot(lows[k, here, :], high, preferred_element_type=jnp.float32)
            whole[here, at] = value
            value_most = jnp.maximum(value_most, jnp.max(jnp.abs(value).reshape(chunk // 8, 8, width), axis=0))
        most[:, pl.ds(k * columns + j * width, width)] = jnp.max(value_most, axis=0, keepdims=True)
    give = near_copy(4, most, far_most)
    give.start()
    for copy in norms:
        copy.wait()
    for i in range(2):
        norm_ref[i, me] = parts[i]
    for i, s, z in peers:
        norm_copy(i, s, z, me, zero).wait_send()
        norm_copy(i, s, z, z * cols + lax.rem(col - s + cols, cols), z).wait_recv()
    for copy in near_copies(me):
        copy.wait_send()
    for copy in near_copies((zeros - 1 - zero) * cols + col):
        copy.wait_recv()
    give.wait()


def local_part(zeros, cols, split, gate, up, low_gate, low_up, high_gate, high_up, train, step):
    rows, columns = gate.shape
    rank = low_gate.shape[1]
    group = zeros * cols
    lanes = 128 if train.shape[0] % 128 == 0 else train.shape[0]
    tall = train.shape[0] // lanes
    width = min(512, columns)
    chunk = min(128, rows)
    dma = pltpu.SemaphoreType.DMA
    hbm, vmem = pl.BlockSpec(memory_space=pltpu.HBM), pl.BlockSpec(memory_space=pltpu.VMEM)
    return pl.pallas_call(
        functools.partial(local_kernel, zeros, cols, width, chunk),
        out_shape=[pltpu.VMEM((rows, columns), jnp.float32)] * 2
        + [pltpu.VMEM((split, columns), up.dtype), pltpu.VMEM((rows - split, columns), up.dtype),
           pltpu.VMEM((2, rank, rows), gate.dtype)]
        + [pltpu.VMEM((1, 2 * columns), jnp.float32)] * 2
        + [pltpu.VMEM((2, group, tall, lanes), jnp.float32)],
        in_specs=[hbm] * 8,
        out_specs=[vmem] * 8,
        scratch_shapes=[
            pltpu.VMEM((rows, columns), gate.dtype),
            pltpu.VMEM((2, rows, rank), gate.dtype),
            pltpu.VMEM((2, rank, rows), gate.dtype),
            pltpu.VMEM((2, rank, columns), gate.dtype),
            pltpu.VMEM((2, tall, lanes), jnp.float32),
            dma((3, columns // width)), dma((2, 2)), dma((2,)),
            dma((2, cols - 1, zeros)), dma((2, cols - 1, zeros)), dma((5,)), dma((5,)),
        ],
        cost_estimate=pl.CostEstimate(flops=2 ** 32, bytes_accessed=2 ** 23, transcendentals=0),
        compiler_params=pltpu.CompilerParams(collective_id=0, has_side_effects=True, vmem_limit_bytes=10 * 2 ** 20),
    )(*[pltpu.with_memory_space_constraint(array, pltpu.HBM) for array in (
        gate, up, low_gate.T, low_up.T, high_gate, high_up, train.reshape(tall, lanes), step.reshape(tall, lanes))])


def write_rows(value_of, chunk, stage, out_ref, base, sems):
    copies = []
    for i in range(stage.shape[0] // chunk):
        here = pl.ds(i * chunk, chunk)
        stage[here, :] = value_of(here).astype(stage.dtype)
        copies.append(pltpu.make_async_copy(
            stage.at[here, :], out_ref.at[pl.ds(pl.multiple_of(base + i * chunk, chunk), chunk), :], sems.at[i]))
        copies[-1].start()
    return copies


def far_value(moved, low_ref, first, high, scale):
    return lambda here: (moved[here, :].astype(jnp.float32) + jnp.dot(
        low_ref[pl.ds(first + here.start, here.size), :], high, preferred_element_type=jnp.float32)) * scale


def most_kernel(zeros, cols, chunk, whole_gate, whole_up, moved, far_lows, high_ref, most, far_most, norm_in,
                gate_out, up_out, column_gate_out, column_up_out, norm_out, low_up, column_up,
                stage, low_gate, column_gate, norm, sems, line_sems):
    zero = lax.axis_index("zero")
    rows, columns = moved.shape
    near, far = zero * rows, (zeros - 1 - zero) * rows
    for k, column in enumerate((column_gate, column_up)):
        at = pl.ds(k * columns, columns)
        column[...] = jnp.maximum(most[:, at], far_most[:, at])
    scale = 1.0 / column_up[...]
    copies = write_rows(lambda here: whole_up[here, :] * scale, chunk, stage.at[0], up_out, near, sems.at[0])
    gate_scale = 1.0 / column_gate[...]
    copies += write_rows(lambda here: whole_gate[here, :] * gate_scale, chunk, stage.at[1], gate_out, near, sems.at[1])
    norm[...] = jnp.concatenate([norm_in[0, g] + norm_in[1, g] for g in range(zeros * cols)], axis=0).astype(norm.dtype)
    for i, (src, dst) in enumerate(((column_gate, column_gate_out), (column_up, column_up_out), (norm, norm_out))):
        copies.append(pltpu.make_async_copy(src, dst, line_sems.at[i]))
        copies[-1].start()
    low_gate[...] = far_lows[0].T
    high = high_ref[...] * jnp.bfloat16(mix_rate)
    copies += write_rows(far_value(moved, low_gate, 0, high, gate_scale), chunk, stage.at[2], gate_out, far, sems.at[2])
    low_up[...] = far_lows[1].T
    for copy in copies:
        copy.wait()


def last_kernel(zeros, chunk, rows, first, moved, low_ref, high_ref, column_ref, up_in, up_out, stage, sems):
    zero = lax.axis_index("zero")
    high, scale = high_ref[...] * jnp.bfloat16(mix_rate), 1.0 / column_ref[...]
    for copy in write_rows(far_value(moved, low_ref, first, high, scale), chunk, stage, up_out,
                           (zeros - 1 - zero) * rows + first, sems):
        copy.wait()


def per_device(zeros, cols, weight_gate, low_gate, high_gate, weight_up, low_up, high_up, norm_train, norm_step):
    rows, columns = weight_gate.shape
    rank = low_gate.shape[1]
    chunk = min(128, rows)
    split = rows * 5 // 8 // chunk * chunk
    if zeros != 2 or not split:
        return plain(zeros, cols, weight_gate, low_gate, high_gate, weight_up, low_up, high_up, norm_train, norm_step)

    def moved(array):
        return lax.ppermute(array, "zero", [(i, zeros - 1 - i) for i in range(zeros)])

    far_gate = moved(weight_gate)
    whole_gate, whole_up, up_first, up_second, far_lows, most, far_most, norm = local_part(
        zeros, cols, split, weight_gate, weight_up, low_gate, low_up, high_gate, high_up, norm_train, norm_step)
    far_up = [moved(up_first), moved(up_second)]
    hbm, vmem = pl.BlockSpec(memory_space=pltpu.HBM), pl.BlockSpec(memory_space=pltpu.VMEM)
    wide = jax.ShapeDtypeStruct((rows * zeros, columns), jnp.bfloat16)
    line = jax.ShapeDtypeStruct((1, columns), jnp.float32)
    group, tall, lanes = norm.shape[1:]
    serving_gate, serving_up, column_gate, column_up, serve_norm, far_low, up_line = pl.pallas_call(
        functools.partial(most_kernel, zeros, cols, chunk),
        out_shape=[wide, wide, line, line, jax.ShapeDtypeStruct((group * tall, lanes), jnp.bfloat16),
                   pltpu.VMEM((rows, rank), low_up.dtype), pltpu.VMEM((1, columns), jnp.float32)],
        in_specs=[vmem] * 8,
        out_specs=[hbm] * 5 + [vmem] * 2,
        scratch_shapes=[pltpu.VMEM((3, rows, columns), jnp.bfloat16), pltpu.VMEM((rows, rank), low_gate.dtype),
                        pltpu.VMEM((1, columns), jnp.float32), pltpu.VMEM((group * tall, lanes), jnp.bfloat16),
                        pltpu.SemaphoreType.DMA((3, rows // chunk)), pltpu.SemaphoreType.DMA((3,))],
        cost_estimate=pl.CostEstimate(flops=2 ** 32, bytes_accessed=3 * 2 ** 22, transcendentals=0),
        compiler_params=pltpu.CompilerParams(vmem_limit_bytes=16 * 2 ** 20),
    )(whole_gate, whole_up, far_gate, far_lows, high_gate, most, far_most, norm)
    for far, first in zip(far_up, (0, split)):
        serving_up = pl.pallas_call(
            functools.partial(last_kernel, zeros, chunk // 2, rows, first),
            out_shape=wide,
            in_specs=[vmem] * 4 + [hbm],
            out_specs=hbm,
            input_output_aliases={4: 0},
            scratch_shapes=[pltpu.VMEM(far.shape, jnp.bfloat16), pltpu.SemaphoreType.DMA((far.shape[0] * 2 // chunk,))],
            cost_estimate=pl.CostEstimate(flops=2 ** 30, bytes_accessed=2 ** 22, transcendentals=0),
            compiler_params=pltpu.CompilerParams(vmem_limit_bytes=16 * 2 ** 20),
        )(far, far_low, high_up, up_line, serving_up)
    return (serving_gate, serving_up, column_gate.reshape(columns), column_up.reshape(columns),
            serve_norm.reshape(group * tall * lanes))


def solution(mesh):
    in_specs = (
        P(("job", "zero"), "cols"),
        P(("job", "zero"), None),
        P("job", "cols"),
        P(("job", "zero"), "cols"),
        P(("job", "zero"), None),
        P("job", "cols"),
        P(("job", "zero", "cols")),
        P(("job", "zero", "cols")),
    )
    out_specs = (
        P("job", "cols"),
        P("job", "cols"),
        P(("job", "cols")),
        P(("job", "cols")),
        P("job"),
    )
    return jax.shard_map(
        functools.partial(per_device, mesh.shape["zero"], mesh.shape["cols"]),
        mesh=mesh, in_specs=in_specs, out_specs=out_specs, check_vma=False
    )
```

```python
import functools

import jax
import jax.numpy as jnp
from jax import lax
from jax.experimental import pallas as pl
from jax.experimental.pallas import tpu as pltpu
from jax.sharding import PartitionSpec as P


mix_rate = 2.0
MESH = pl.DeviceIdType.MESH


def first_kernel(zeros, cols, lows, weight_ref, *refs):
    train_ref, step_ref = refs[:2]
    low_refs = refs[2:2 + lows]
    norm_ref = refs[2 + lows]
    got_refs = refs[3 + lows:3 + 2 * lows]
    moved_refs = refs[3 + 2 * lows:2 + 2 * lows + zeros]
    refs = refs[2 + 2 * lows + zeros:]
    landed = refs[:lows]
    mine, slots, norm_send, norm_recv, low_send, low_recv, weight_send, weight_recv = refs[lows:]
    group = zeros * cols
    zero, col = lax.axis_index("zero"), lax.axis_index("cols")
    me = zero * cols + col

    def device(rank):
        return {"zero": rank // cols, "cols": lax.rem(rank, cols)}

    barrier = pltpu.get_barrier_semaphore()
    for s in range(1, group):
        pl.semaphore_signal(barrier, inc=1, device_id=device(lax.rem(me + s, group)), device_id_type=MESH)
    mine[...] = train_ref[...] + step_ref[...]
    pl.semaphore_wait(barrier, group - 1)

    copies = []
    for s in range(1, zeros):
        for k in range(lows):
            copies.append(pltpu.make_async_remote_copy(
                src_ref=low_refs[k], dst_ref=landed[k].at[s - 1],
                send_sem=low_send.at[k, s - 1], recv_sem=low_recv.at[k, s - 1],
                device_id={"zero": lax.rem(zero + s, zeros), "cols": col}, device_id_type=MESH))
            copies[-1].start()
    for s in range(1, zeros):
        copies.append(pltpu.make_async_remote_copy(
            src_ref=weight_ref, dst_ref=moved_refs[s - 1],
            send_sem=weight_send.at[s - 1], recv_sem=weight_recv.at[s - 1],
            device_id={"zero": lax.rem(zero + s, zeros), "cols": col}, device_id_type=MESH))
    for s in range(1, group):
        copy = pltpu.make_async_remote_copy(
            src_ref=mine, dst_ref=slots.at[me],
            send_sem=norm_send.at[s - 1], recv_sem=norm_recv.at[s - 1],
            device_id=device(lax.rem(me + s, group)), device_id_type=MESH)
        copy.start()
        copies.append(copy)
    for copy in copies[lows * (zeros - 1):(1 + lows) * (zeros - 1)]:
        copy.start()
    for k in range(lows):
        got_refs[k][0] = low_refs[k][...].T
    for copy in copies:
        copy.wait()
    for k in range(lows):
        for s in range(1, zeros):
            got_refs[k][s] = landed[k][s - 1].T
    slots[me] = mine[...]
    norm_ref[...] = jnp.concatenate([slots[g] for g in range(group)], axis=0).astype(norm_ref.dtype)


def exchange_first(zeros, cols, weight, train, step, lows):
    group = zeros * cols
    lanes = 128 if train.shape[0] % 128 == 0 else train.shape[0]
    tall = train.shape[0] // lanes
    outs = pl.pallas_call(
        functools.partial(first_kernel, zeros, cols, len(lows)),
        out_shape=[jax.ShapeDtypeStruct((group * tall, lanes), jnp.bfloat16)]
        + [jax.ShapeDtypeStruct((zeros,) + low.shape, low.dtype) for low in lows]
        + [jax.ShapeDtypeStruct(weight.shape, weight.dtype)] * (zeros - 1),
        in_specs=[pl.BlockSpec(memory_space=pl.ANY)] + [pl.BlockSpec(memory_space=pltpu.VMEM)] * (2 + len(lows)),
        out_specs=[pl.BlockSpec(memory_space=pltpu.VMEM)] * (1 + len(lows))
        + [pl.BlockSpec(memory_space=pl.ANY)] * (zeros - 1),
        scratch_shapes=[
            pltpu.VMEM((zeros - 1,) + low.shape[::-1], low.dtype) for low in lows
        ] + [
            pltpu.VMEM((tall, lanes), jnp.float32),
            pltpu.VMEM((group, tall, lanes), jnp.float32),
            pltpu.SemaphoreType.DMA((group - 1,)),
            pltpu.SemaphoreType.DMA((group - 1,)),
            pltpu.SemaphoreType.DMA((len(lows), zeros - 1)),
            pltpu.SemaphoreType.DMA((len(lows), zeros - 1)),
            pltpu.SemaphoreType.DMA((zeros - 1,)),
            pltpu.SemaphoreType.DMA((zeros - 1,)),
        ],
        cost_estimate=pl.CostEstimate(flops=0, bytes_accessed=2 ** 22, transcendentals=0),
        compiler_params=pltpu.CompilerParams(collective_id=0, has_side_effects=True),
    )(weight, train.reshape(tall, lanes), step.reshape(tall, lanes), *[low.T for low in lows])
    return outs[0].reshape(group * tall * lanes), outs[1:1 + len(lows)], outs[1 + len(lows):]


def merge_kernel(zeros, chunk, *refs):
    weight_refs = refs[:zeros]
    low_ref, high_ref, out_ref, column_ref, whole = refs[zeros:]
    zero = lax.axis_index("zero")
    rows, width = weight_refs[0].shape
    high = high_ref[...] * jnp.bfloat16(mix_rate)
    most = jnp.zeros((8, width), jnp.float32)
    for s in range(zeros):
        def step(i, most, s=s):
            at = pl.ds(pl.multiple_of(i * chunk, chunk), chunk)
            low = low_ref[s, at, :]
            value = weight_refs[s][at, :].astype(jnp.float32) + jnp.dot(
                low, high, preferred_element_type=jnp.float32)
            whole[s, at, :] = value
            return jnp.maximum(most, jnp.max(jnp.abs(value).reshape(chunk // 8, 8, width), axis=0))

        most = lax.fori_loop(0, rows // chunk, step, most, unroll=True)
    column = jnp.max(most, axis=0, keepdims=True)
    column_ref[...] = column
    scale = 1.0 / column
    for s in range(zeros):
        base = lax.rem(zero - s + zeros, zeros) * rows

        def put(i, carry, s=s, base=base):
            start = pl.multiple_of(i * chunk, chunk)
            out_ref[pl.ds(pl.multiple_of(base + start, chunk), chunk), :] = (
                whole[s, pl.ds(start, chunk), :] * scale).astype(out_ref.dtype)
            return carry

        lax.fori_loop(0, rows // chunk, put, 0, unroll=True)


def merge(zeros, weights, low, high):
    rows, columns = weights[0].shape
    rank = low.shape[2]
    width = min(512, columns)
    chunk = min(128, rows)
    serving, column = pl.pallas_call(
        functools.partial(merge_kernel, zeros, chunk),
        grid=(columns // width,),
        out_shape=[
            jax.ShapeDtypeStruct((rows * zeros, columns), jnp.bfloat16),
            jax.ShapeDtypeStruct((1, columns), jnp.float32),
        ],
        in_specs=[pl.BlockSpec((rows, width), lambda j: (0, j))] * zeros + [
            pl.BlockSpec((zeros, rows, rank), lambda j: (0, 0, 0)),
            pl.BlockSpec((rank, width), lambda j: (0, j)),
        ],
        out_specs=[
            pl.BlockSpec((rows * zeros, width), lambda j: (0, j)),
            pl.BlockSpec((1, width), lambda j: (0, j)),
        ],
        scratch_shapes=[pltpu.VMEM((zeros, rows, width), jnp.float32)],
        cost_estimate=pl.CostEstimate(
            flops=2 * rows * zeros * columns * rank,
            bytes_accessed=4 * rows * zeros * columns, transcendentals=0),
        compiler_params=pltpu.CompilerParams(dimension_semantics=("arbitrary",), vmem_limit_bytes=60 * 2 ** 20),
    )(*weights, low, high)
    return serving, column.reshape(columns)


def plain(zeros, cols, weight_gate, low_gate, high_gate, weight_up, low_up, high_up, norm_train, norm_step):
    def moved(array):
        return [array] + [
            lax.ppermute(array, "zero", [(i, (i + s) % zeros) for i in range(zeros)])
            for s in range(1, zeros)
        ]

    serve_norm, (all_gate, all_up), gates = exchange_first(
        zeros, cols, weight_gate, norm_train, norm_step, (low_gate, low_up))
    weight_up, all_up = lax.optimization_barrier((weight_up, all_up))
    ups = moved(weight_up)
    serving_gate, column_gate = merge(zeros, [weight_gate, *gates], all_gate, high_gate)
    serving_up, column_up = merge(zeros, ups, all_up, high_up)
    return (serving_gate, serving_up, column_gate, column_up, serve_norm)


def local_kernel(zeros, cols, width, chunk, gate_ref, up_ref, low_gate_ref, low_up_ref, high_gate_ref, high_up_ref,
                 train_ref, step_ref, whole_gate, whole_up, up_first, up_second, far_lows, most, far_most, norm_ref,
                 raw, lows, lows_t, highs, parts, weight_sems, small_sems, norm_sems, norm_send, norm_recv,
                 near_send, near_recv):
    zero, col = lax.axis_index("zero"), lax.axis_index("cols")
    me = zero * cols + col
    rows, columns = raw.shape
    pieces = columns // width
    split = up_first.shape[0]
    ahead = 3

    barrier = pltpu.get_barrier_semaphore()
    for z in range(1, zeros):
        pl.semaphore_signal(barrier, inc=1, device_id={"zero": lax.rem(zero + z, zeros), "cols": col}, device_id_type=MESH)
    for s in range(1, cols):
        for z in range(zeros):
            pl.semaphore_signal(barrier, inc=1, device_id={"zero": z, "cols": lax.rem(col + s, cols)}, device_id_type=MESH)

    loads = []
    for j in range(pieces):
        at = pl.ds(j * width, width)
        loads.append([pltpu.make_async_copy(gate_ref.at[:, at], raw.at[:, at], weight_sems.at[0, j])])
    for j in range(pieces):
        at = pl.ds(j * width, width)
        loads.append([pltpu.make_async_copy(up_ref.at[pl.ds(0, split), at], up_first.at[:, at], weight_sems.at[1, j]),
                      pltpu.make_async_copy(up_ref.at[pl.ds(split, rows - split), at], up_second.at[:, at], weight_sems.at[2, j])])
    small = []
    for k, (low, high) in enumerate(((low_gate_ref, high_gate_ref), (low_up_ref, high_up_ref))):
        small.append(pltpu.make_async_copy(low, lows_t.at[k], small_sems.at[k, 0]))
        small.append(pltpu.make_async_copy(high, highs.at[k], small_sems.at[k, 1]))
    norms = [pltpu.make_async_copy(ref, parts.at[i], norm_sems.at[i]) for i, ref in enumerate((train_ref, step_ref))]
    for copy in norms + small[:2] + sum(loads[:ahead], []) + small[2:]:
        copy.start()

    def norm_copy(i, s, z, rank, recv):
        return pltpu.make_async_remote_copy(
            src_ref=(train_ref, step_ref)[i], dst_ref=norm_ref.at[i, rank],
            send_sem=norm_send.at[i, s - 1, z], recv_sem=norm_recv.at[i, s - 1, recv],
            device_id={"zero": z, "cols": lax.rem(col + s, cols)}, device_id_type=MESH)

    def near_copy(i, src, dst):
        return pltpu.make_async_remote_copy(
            src_ref=src, dst_ref=dst, send_sem=near_send.at[i], recv_sem=near_recv.at[i],
            device_id={"zero": zeros - 1 - zero, "cols": col}, device_id_type=MESH)

    def near_copies(rank):
        return [near_copy(0, low_gate_ref, far_lows.at[0]), near_copy(1, low_up_ref, far_lows.at[1]),
                near_copy(2, train_ref, norm_ref.at[0, rank]), near_copy(3, step_ref, norm_ref.at[1, rank])]

    peers = [(i, s, z) for s in range(cols - 1, 0, -1) for z in range(zeros) for i in range(2)]
    entry = jnp.maximum(2 * pieces * (cols - 1 - col) // cols - 1, 0)
    for n in range(2 * pieces):
        @pl.when(entry == n)
        def _():
            pl.semaphore_wait(barrier, zeros * cols - 1)
            for i, s, z in peers:
                norm_copy(i, s, z, me, zero).start()
            for copy in near_copies(me):
                copy.start()

        k, j = n // pieces, n % pieces
        if j == 0:
            small[2 * k].wait()
            small[2 * k + 1].wait()
            lows[k] = lows_t[k].T
        for copy in loads[n]:
            copy.wait()
        if n + ahead < len(loads):
            for copy in loads[n + ahead]:
                copy.start()
        at = pl.ds(j * width, width)
        high = highs[k, :, at] * jnp.bfloat16(mix_rate)
        whole = (whole_gate, whole_up)[k]
        value_most = jnp.zeros((8, width), jnp.float32)
        for i in range(rows // chunk):
            here = pl.ds(i * chunk, chunk)
            if k == 0:
                part = raw[here, at]
            elif i * chunk < split:
                part = up_first[here, at]
            else:
                part = up_second[pl.ds(i * chunk - split, chunk), at]
            value = part.astype(jnp.float32) + jnp.dot(lows[k, here, :], high, preferred_element_type=jnp.float32)
            whole[here, at] = value
            value_most = jnp.maximum(value_most, jnp.max(jnp.abs(value).reshape(chunk // 8, 8, width), axis=0))
        most[:, pl.ds(k * columns + j * width, width)] = jnp.max(value_most, axis=0, keepdims=True)
    give = near_copy(4, most, far_most)
    give.start()
    for copy in norms:
        copy.wait()
    for i in range(2):
        norm_ref[i, me] = parts[i]
    for i, s, z in peers:
        norm_copy(i, s, z, me, zero).wait_send()
        norm_copy(i, s, z, z * cols + lax.rem(col - s + cols, cols), z).wait_recv()
    for copy in near_copies(me):
        copy.wait_send()
    for copy in near_copies((zeros - 1 - zero) * cols + col):
        copy.wait_recv()
    give.wait()


def local_part(zeros, cols, split, gate, up, low_gate, low_up, high_gate, high_up, train, step):
    rows, columns = gate.shape
    rank = low_gate.shape[1]
    group = zeros * cols
    lanes = 128 if train.shape[0] % 128 == 0 else train.shape[0]
    tall = train.shape[0] // lanes
    width = min(512, columns)
    chunk = min(128, rows)
    dma = pltpu.SemaphoreType.DMA
    hbm, vmem = pl.BlockSpec(memory_space=pltpu.HBM), pl.BlockSpec(memory_space=pltpu.VMEM)
    return pl.pallas_call(
        functools.partial(local_kernel, zeros, cols, width, chunk),
        out_shape=[pltpu.VMEM((rows, columns), jnp.float32)] * 2
        + [pltpu.VMEM((split, columns), up.dtype), pltpu.VMEM((rows - split, columns), up.dtype),
           pltpu.VMEM((2, rank, rows), gate.dtype)]
        + [pltpu.VMEM((1, 2 * columns), jnp.float32)] * 2
        + [pltpu.VMEM((2, group, tall, lanes), jnp.float32)],
        in_specs=[hbm] * 8,
        out_specs=[vmem] * 8,
        scratch_shapes=[
            pltpu.VMEM((rows, columns), gate.dtype),
            pltpu.VMEM((2, rows, rank), gate.dtype),
            pltpu.VMEM((2, rank, rows), gate.dtype),
            pltpu.VMEM((2, rank, columns), gate.dtype),
            pltpu.VMEM((2, tall, lanes), jnp.float32),
            dma((3, columns // width)), dma((2, 2)), dma((2,)),
            dma((2, cols - 1, zeros)), dma((2, cols - 1, zeros)), dma((5,)), dma((5,)),
        ],
        cost_estimate=pl.CostEstimate(flops=2 ** 32, bytes_accessed=2 ** 23, transcendentals=0),
        compiler_params=pltpu.CompilerParams(collective_id=0, has_side_effects=True, vmem_limit_bytes=10 * 2 ** 20),
    )(*[pltpu.with_memory_space_constraint(array, pltpu.HBM) for array in (
        gate, up, low_gate.T, low_up.T, high_gate, high_up, train.reshape(tall, lanes), step.reshape(tall, lanes))])


def write_rows(value_of, chunk, stage, out_ref, base, sems):
    copies = []
    for i in range(stage.shape[0] // chunk):
        here = pl.ds(i * chunk, chunk)
        stage[here, :] = value_of(here).astype(stage.dtype)
        copies.append(pltpu.make_async_copy(
            stage.at[here, :], out_ref.at[pl.ds(pl.multiple_of(base + i * chunk, chunk), chunk), :], sems.at[i]))
        copies[-1].start()
    return copies


def far_value(moved, low_ref, first, high, scale):
    return lambda here: (moved[here, :].astype(jnp.float32) + jnp.dot(
        low_ref[pl.ds(first + here.start, here.size), :], high, preferred_element_type=jnp.float32)) * scale


def most_kernel(zeros, cols, chunk, whole_gate, whole_up, moved, far_lows, high_ref, most, far_most, norm_in,
                gate_out, up_out, column_gate_out, column_up_out, norm_out, low_up, scale_up,
                stage, low_gate, column_gate, column_up, norm, sems, line_sems):
    zero = lax.axis_index("zero")
    rows, columns = moved.shape
    near, far = zero * rows, (zeros - 1 - zero) * rows
    for k, column in enumerate((column_gate, column_up)):
        at = pl.ds(k * columns, columns)
        column[...] = jnp.maximum(most[:, at], far_most[:, at])
    scale = 1.0 / column_up[...]
    scale_up[...] = scale
    copies = write_rows(lambda here: whole_up[here, :] * scale, chunk, stage.at[0], up_out, near, sems.at[0])
    gate_scale = 1.0 / column_gate[...]
    copies += write_rows(lambda here: whole_gate[here, :] * gate_scale, chunk, stage.at[1], gate_out, near, sems.at[1])
    norm[...] = jnp.concatenate([norm_in[0, g] + norm_in[1, g] for g in range(zeros * cols)], axis=0).astype(norm.dtype)
    for i, (src, dst) in enumerate(((column_gate, column_gate_out), (column_up, column_up_out), (norm, norm_out))):
        copies.append(pltpu.make_async_copy(src, dst, line_sems.at[i]))
        copies[-1].start()
    low_gate[...] = far_lows[0].T
    high = high_ref[...] * jnp.bfloat16(mix_rate)
    copies += write_rows(far_value(moved, low_gate, 0, high, gate_scale), chunk, stage.at[2], gate_out, far, sems.at[2])
    low_up[...] = far_lows[1].T
    for copy in copies:
        copy.wait()


def last_kernel(zeros, chunk, rows, first, moved, low_ref, high_ref, column_ref, up_in, up_out, stage, sems):
    zero = lax.axis_index("zero")
    high, scale = high_ref[...] * jnp.bfloat16(mix_rate), column_ref[...]
    for copy in write_rows(far_value(moved, low_ref, first, high, scale), chunk, stage, up_out,
                           (zeros - 1 - zero) * rows + first, sems):
        copy.wait()


def per_device(zeros, cols, weight_gate, low_gate, high_gate, weight_up, low_up, high_up, norm_train, norm_step):
    rows, columns = weight_gate.shape
    rank = low_gate.shape[1]
    chunk = min(128, rows)
    split = rows * 5 // 8 // chunk * chunk
    if zeros != 2 or not split:
        return plain(zeros, cols, weight_gate, low_gate, high_gate, weight_up, low_up, high_up, norm_train, norm_step)

    def moved(array):
        return lax.ppermute(array, "zero", [(i, zeros - 1 - i) for i in range(zeros)])

    far_gate = moved(weight_gate)
    whole_gate, whole_up, up_first, up_second, far_lows, most, far_most, norm = local_part(
        zeros, cols, split, weight_gate, weight_up, low_gate, low_up, high_gate, high_up, norm_train, norm_step)
    far_up = [moved(up_first), moved(up_second)]
    hbm, vmem = pl.BlockSpec(memory_space=pltpu.HBM), pl.BlockSpec(memory_space=pltpu.VMEM)
    wide = jax.ShapeDtypeStruct((rows * zeros, columns), jnp.bfloat16)
    line = jax.ShapeDtypeStruct((1, columns), jnp.float32)
    group, tall, lanes = norm.shape[1:]
    serving_gate, serving_up, column_gate, column_up, serve_norm, far_low, up_line = pl.pallas_call(
        functools.partial(most_kernel, zeros, cols, chunk),
        out_shape=[wide, wide, line, line, jax.ShapeDtypeStruct((group * tall, lanes), jnp.bfloat16),
                   pltpu.VMEM((rows, rank), low_up.dtype), pltpu.VMEM((1, columns), jnp.float32)],
        in_specs=[vmem] * 8,
        out_specs=[hbm] * 5 + [vmem] * 2,
        scratch_shapes=[pltpu.VMEM((3, rows, columns), jnp.bfloat16), pltpu.VMEM((rows, rank), low_gate.dtype),
                        pltpu.VMEM((1, columns), jnp.float32), pltpu.VMEM((1, columns), jnp.float32),
                        pltpu.VMEM((group * tall, lanes), jnp.bfloat16),
                        pltpu.SemaphoreType.DMA((3, rows // chunk)), pltpu.SemaphoreType.DMA((3,))],
        cost_estimate=pl.CostEstimate(flops=2 ** 32, bytes_accessed=3 * 2 ** 22, transcendentals=0),
        compiler_params=pltpu.CompilerParams(vmem_limit_bytes=16 * 2 ** 20),
    )(whole_gate, whole_up, far_gate, far_lows, high_gate, most, far_most, norm)
    for far, first in zip(far_up, (0, split)):
        serving_up = pl.pallas_call(
            functools.partial(last_kernel, zeros, chunk // 2, rows, first),
            out_shape=wide,
            in_specs=[vmem] * 4 + [hbm],
            out_specs=hbm,
            input_output_aliases={4: 0},
            scratch_shapes=[pltpu.VMEM(far.shape, jnp.bfloat16), pltpu.SemaphoreType.DMA((far.shape[0] * 2 // chunk,))],
            cost_estimate=pl.CostEstimate(flops=2 ** 30, bytes_accessed=2 ** 22, transcendentals=0),
            compiler_params=pltpu.CompilerParams(vmem_limit_bytes=16 * 2 ** 20),
        )(far, far_low, high_up, up_line, serving_up)
    return (serving_gate, serving_up, column_gate.reshape(columns), column_up.reshape(columns),
            serve_norm.reshape(group * tall * lanes))


def solution(mesh):
    in_specs = (
        P(("job", "zero"), "cols"),
        P(("job", "zero"), None),
        P("job", "cols"),
        P(("job", "zero"), "cols"),
        P(("job", "zero"), None),
        P("job", "cols"),
        P(("job", "zero", "cols")),
        P(("job", "zero", "cols")),
    )
    out_specs = (
        P("job", "cols"),
        P("job", "cols"),
        P(("job", "cols")),
        P(("job", "cols")),
        P("job"),
    )
    return jax.shard_map(
        functools.partial(per_device, mesh.shape["zero"], mesh.shape["cols"]),
        mesh=mesh, in_specs=in_specs, out_specs=out_specs, check_vma=False
    )
```
